32 devices in a mesh: batch: 8 (over z, y), rows: 4 (over x, core).
Axes of the slice: x: 2, y: 2, z: 4, core: 2. Of those that a mesh axis runs over, the one named last changes fastest.
Arguments:
- features: bfloat16 [192, 14, 14, 1024], P(('batch', 'rows')), may hold values from -12 to 12
- grads: bfloat16 [192, 14, 14, 256], P(('batch', 'rows')), may hold values from -12 to 12
- kernel: bfloat16 [3, 3, 256, 1024], replicated, may hold values from -0.125 to 0.125
- vectors: float32 [16, 64, 64], replicated, may hold values from -1 to 1, as said below
- values: float32 [16, 64], replicated, may hold values from 0.05 to 2
Outputs:
- input_grad: bfloat16 [192, 14, 14, 1024], P(('batch', 'rows'))
- kernel_grad: float32 [1024, 3, 3, 256], P(('batch', 'rows'))
The draws below stay inside these ranges and needn't reach their ends.
Inputs may be any that keep to these rules, and one draw needn't show every extreme that they name: `vectors`: each group's matrix is orthogonal.
All inputs are finite; a program needn't handle non-finite values.
Results may differ from the reference program's by a relative error of at most 0.015.
Values sent between devices are 32-bit elements; how exact they have to be, the bound alone decides.
A program may use at most 128 MiB of HBM per device.

```python
import math
import jax
import jax.numpy as jnp
from jax import lax

D = 1024
GSIZE = 64
COUT = 256
WD = 14
HEIGHT = 14
IMG_DEV = 6
GROUPS = 16
IMAGES = 192
DEVICES = 32


def draw_features(key, part):
    key_offset, key_spread, key_noise = jax.random.split(jax.random.fold_in(key, 11), 3)
    offsets = 0.5 * jax.random.normal(key_offset, (D,), jnp.float32)
    spread = jnp.exp(jax.random.uniform(key_spread, (D,), jnp.float32, math.log(0.5), math.log(2.0)))
    ramp = 1.0 + 2.0 * jnp.arange(IMAGES, dtype=jnp.float32) / max(IMAGES - 1, 1)
    noise = jax.random.normal(key_noise, (IMAGES, HEIGHT, WD, D), jnp.float32)
    result = offsets * ramp[:, None, None, None] + spread * noise
    return jnp.clip(result, -12.0, 12.0).astype(jnp.bfloat16)


def draw_grads(key, part):
    key_offset, key_spread, key_noise = jax.random.split(jax.random.fold_in(key, 23), 3)
    offsets = 0.3 * jax.random.normal(key_offset, (COUT,), jnp.float32)
    spread = jnp.exp(jax.random.uniform(key_spread, (COUT,), jnp.float32, math.log(0.5), math.log(2.0)))
    ramp = 1.0 + 2.0 * jnp.arange(IMAGES, dtype=jnp.float32) / max(IMAGES - 1, 1)
    noise = jax.random.normal(key_noise, (IMAGES, HEIGHT, WD, COUT), jnp.float32)
    result = offsets * ramp[:, None, None, None] + spread * noise
    return jnp.clip(result, -12.0, 12.0).astype(jnp.bfloat16)


def draw_vectors(key, part):
    matrices = jax.random.normal(jax.random.fold_in(key, 37), (GROUPS, GSIZE, GSIZE), jnp.float32)
    basis, unused = jnp.linalg.qr(matrices)
    return basis.astype(jnp.float32)


def normal_values(rng, shape, deviation, most, kind=jnp.bfloat16):
    return jnp.clip(deviation * jax.random.normal(rng, shape, jnp.float32), -most, most).astype(kind)


def setup_inputs(seed: int = 0) -> dict:
    keys = jax.random.split(jax.random.key(seed), 6)
    features = draw_features(jax.random.fold_in(keys[5], 71), 0)
    grads = draw_grads(jax.random.fold_in(keys[5], 71), 0)
    kernel = normal_values(keys[2], (3, 3, COUT, D), (9 * COUT) ** -0.5, 0.125)
    vectors = draw_vectors(jax.random.fold_in(keys[5], 71), 0)
    values = jnp.clip(jnp.exp(jax.random.uniform(keys[4], (GROUPS, GSIZE), jnp.float32, math.log(0.05), math.log(2.0))), 0.05, 2.0)
    return {"features": features, "grads": grads, "kernel": kernel, "vectors": vectors, "values": values}


highest = lax.Precision.HIGHEST

def whitening(vectors, values):
    scales = lax.rsqrt(values)
    whiten = jnp.einsum('gij,gj,gkj->gik', vectors, scales, vectors, precision=highest)
    return (scales, whiten)

def block_matrix(blocks):
    groups, group_size = (blocks.shape[0], blocks.shape[1])
    identity = jnp.eye(groups, dtype=jnp.float32)
    full = jnp.einsum('gh,gij->gihj', identity, blocks, precision=highest)
    return full.reshape(groups * group_size, groups * group_size)

def diagonal_blocks(full, groups, group_size):
    shaped = full.reshape(groups, group_size, groups, group_size)
    index = jnp.arange(groups)
    return shaped[index, :, index, :]

def gather_columns(padded, slab_rows, columns_count):
    outputs = padded.shape[3]
    pieces = [padded[:, 2 - shift_row:2 - shift_row + slab_rows, 2 - shift_col:2 - shift_col + columns_count, :] for shift_row in range(3) for shift_col in range(3)]
    return jnp.concatenate(pieces, axis=3).reshape(-1, 9 * outputs)

def reference(features, grads, kernel, vectors, values):
    group_size = values.shape[1]
    groups = values.shape[0]
    channels = features.shape[3]
    outputs = grads.shape[3]
    pixel_total = 1.0 * features.shape[0] * features.shape[1] * features.shape[2]
    feature_blocks = features.reshape(DEVICES, IMG_DEV, HEIGHT, WD, channels)
    grad_blocks = grads.reshape(DEVICES, IMG_DEV, HEIGHT, WD, outputs)
    kernel_flat = kernel.reshape(9 * outputs, channels)
    scales, whiten = whitening(vectors, values)
    whiten_low = block_matrix(whiten).astype(jnp.bfloat16)

    def add_sums(carry, block):
        return (carry + lax.optimization_barrier(jnp.sum(block.reshape(-1, channels), axis=0, dtype=jnp.float32)), None)
    sum_feature, unused = lax.scan(add_sums, jnp.zeros((channels,), jnp.float32), feature_blocks)
    channel_mean = sum_feature / pixel_total

    def block_terms(feature_block, grad_block):
        flat = feature_block.reshape(-1, channels)
        centered_low = (flat.astype(jnp.float32) - channel_mean).astype(jnp.bfloat16)
        padded = jnp.pad(grad_block, ((0, 0), (1, 1), (1, 1), (0, 0)))
        columns = gather_columns(padded, HEIGHT, WD)
        back_grad = jnp.dot(columns.astype(jnp.float32), kernel_flat.astype(jnp.float32), preferred_element_type=jnp.float32)
        return (flat, centered_low, columns, back_grad)

    def accumulate(carry, blocks):
        cov_part, back_part, weight_part = carry
        flat, centered_low, columns, back_grad = block_terms(blocks[0], blocks[1])
        whitened = jnp.dot(centered_low.astype(jnp.float32), whiten_low.astype(jnp.float32), preferred_element_type=jnp.float32).astype(jnp.bfloat16)
        back_low = back_grad.astype(jnp.bfloat16)
        cov_part = cov_part + lax.dot_general(flat.astype(jnp.float32), back_low.astype(jnp.float32), (((0,), (0,)), ((), ())), preferred_element_type=jnp.float32)
        back_part = back_part + lax.optimization_barrier(jnp.sum(back_grad, axis=0))
        weight_part = weight_part + lax.dot_general(whitened.astype(jnp.float32), columns.astype(jnp.float32), (((0,), (0,)), ((), ())), preferred_element_type=jnp.float32)
        return ((cov_part, back_part, weight_part), None)
    start_carry = (jnp.zeros((channels, channels), jnp.float32), jnp.zeros((channels,), jnp.float32), jnp.zeros((channels, 9 * outputs), jnp.float32))
    totals, unused = lax.scan(accumulate, start_carry, (feature_blocks, grad_blocks))
    raw_full, back_total, weight_total = totals
    raw_cov = diagonal_blocks(raw_full, groups, group_size)
    cov_grad = raw_cov - channel_mean.reshape(groups, group_size)[:, :, None] * back_total.reshape(groups, group_size)[:, None, :]
    rotated = jnp.einsum('gki,gkl,glj->gij', vectors, cov_grad, vectors, precision=highest)
    symmetric = 0.5 * (rotated + jnp.swapaxes(rotated, 1, 2))
    roots = jnp.sqrt(values)
    factor = -(scales[:, :, None] * scales[:, None, :]) / (roots[:, :, None] + roots[:, None, :])
    sigma_grad = jnp.einsum('gik,gkl,gjl->gij', vectors, symmetric * factor, vectors, precision=highest)
    sigma_low = block_matrix(2.0 / pixel_total * sigma_grad).astype(jnp.bfloat16)
    stacked = jnp.concatenate([whiten_low, sigma_low], axis=0)

    def input_block(blocks):
        flat, centered_low, columns, back_grad = block_terms(blocks[0], blocks[1])
        shifted_low = (back_grad - back_total / pixel_total).astype(jnp.bfloat16)
        joined = jnp.concatenate([shifted_low, centered_low], axis=1)
        result = jnp.dot(joined.astype(jnp.float32), stacked.astype(jnp.float32), preferred_element_type=jnp.float32)
        return result.reshape(IMG_DEV, HEIGHT, WD, channels).astype(jnp.bfloat16)
    input_grad = lax.map(input_block, (feature_blocks, grad_blocks)).reshape(features.shape)
    kernel_grad = weight_total.reshape(channels, 3, 3, outputs)
    return (input_grad, kernel_grad)
```

```python
import functools
import jax
import jax.numpy as jnp
from jax import lax
from jax.experimental import pallas as pl
from jax.experimental.pallas import tpu as pltpu
from jax.sharding import PartitionSpec as P

highest = lax.Precision.HIGHEST
F32, BF16 = jnp.float32, jnp.bfloat16
LANES = 128
VMEM_LIMIT = 63 * 1024 * 1024


def round_up(n, m):
    return (n + m - 1) // m * m


def bit_orders(bits):
    rest = list(range(1, bits))
    first = [0] + rest
    second = [0] + rest[1:2] + rest[:1] + rest[2:]
    third = [0] + rest[2:3] + rest[:2] + rest[3:]
    return [first, second, third]


def slot_of(index, order):
    slot = 0
    count = len(order)
    for step, bit in enumerate(order):
        slot = slot + (index // 2**bit) % 2 * 2 ** (count - 1 - step)
    return slot


def general_kernel(
    sizes, f_ref, g_ref, k_hbm, v_ref, sv_ref, o_ref, share_ref,
    fp, ft, cols, gpad, k_ref, back, w_ref, s_ref, flat, small, total, column, pieces,
    k_sem, send_sem, recv_sem, *scratch
):
    (nb, nr, images, height, width, wide, channels, outputs, per, orders, streams, pixel_total) = sizes
    rows = images * height * wide
    kp = fp.shape[0]
    blocks = channels // LANES
    taps = 3 * outputs
    part_width = 3 * taps // streams
    bits = len(orders[0])
    count = 2**bits
    rp = small.shape[1]
    half = LANES // 2
    base = channels // 2
    image_rows = height * wide
    batch = lax.axis_index("batch")
    row = lax.axis_index("rows")
    index = batch * nr + row

    def bit_of(bit):
        return (index // 2**bit) % 2

    def partner(bit):
        sign = 1 - 2 * bit_of(bit)
        if 2**bit < nr:
            return (batch, row + sign * 2**bit)
        return (batch + sign * (2**bit // nr), row)

    barrier = pltpu.get_barrier_semaphore()
    for bit in range(bits):
        pl.semaphore_signal(
            barrier, inc=1, device_id=partner(bit), device_id_type=pl.DeviceIdType.MESH
        )
    k_copy = pltpu.make_async_copy(k_hbm, k_ref, k_sem)
    k_copy.start()

    fp[pl.ds(rows, kp - rows), :] = jnp.zeros((kp - rows, channels), BF16)
    cols[pl.ds(rows, kp - rows), :] = jnp.zeros((kp - rows, 3 * taps), BF16)
    gpad[...] = jnp.zeros(gpad.shape, F32)

    @pl.loop(0, images)
    def _(b):
        gpad[pl.ds(1, height), pl.ds(1, width), :] = g_ref[b].astype(F32)
        for h in range(height):
            at = pl.multiple_of((b * height + h) * wide, 16)
            fp[pl.ds(at, wide), :] = jnp.zeros((wide, channels), BF16)
            fp[pl.ds(at, width), :] = f_ref[b, h]
        at = pl.multiple_of(b * image_rows, 16)
        for c in range(3):
            shifted = gpad[:, 2 - c : 2 - c + wide, :].astype(BF16)
            for a in range(3):
                first = a * taps + c * outputs
                cols[pl.ds(at, image_rows), first : first + outputs] = shifted[
                    2 - a : 2 - a + height
                ].reshape(image_rows, outputs)

    @pl.loop(0, blocks)
    def _(k):
        at = pl.ds(pl.multiple_of(k * LANES, LANES), LANES)
        ft[at, :] = fp[:, at].T
        v = v_ref[k]
        w_ref[k] = lax.dot_general(
            v * sv_ref[0, pl.ds(k, 1), :], v, (((1,), (1,)), ((), ())),
            precision=highest, preferred_element_type=F32,
        ).astype(BF16)

    position = lax.broadcasted_iota(jnp.int32, (kp, 1), 0)
    valid = (position % wide < width) & (position < rows)
    lane = lax.broadcasted_iota(jnp.int32, (8, kp), 1)
    ones = jnp.where((lane % wide < width) & (lane < rows), 1.0, 0.0).astype(BF16)
    low_lane = lax.broadcasted_iota(jnp.int32, (half, LANES), 1) < half
    flat[pl.ds(base, flat.shape[0] - base), :] = jnp.zeros((flat.shape[0] - base, LANES), F32)

    def copy(src, dst, s, t, bit):
        c = pltpu.make_async_remote_copy(
            src_ref=src,
            dst_ref=dst,
            send_sem=send_sem.at[s, t],
            recv_sem=recv_sem.at[s, t],
            device_id=partner(bit),
            device_id_type=pl.DeviceIdType.MESH,
        )
        c.start()
        return c

    sources = [pieces.at[s] for s in range(streams)] + [small]
    buffers = [[scratch[s * bits + t] for t in range(bits)] for s in range(streams + 1)]
    all_orders = [orders[s % 3] for s in range(streams)] + [orders[0]]
    flights = {}

    def begin(s, t):
        bit = all_orders[s][t]
        size = count >> (t + 1)
        src = sources[s] if t == 0 else buffers[s][t - 1]
        flights[s] = copy(
            src.at[pl.ds((1 - bit_of(bit)) * size, size)], buffers[s][t], s, t, bit
        )

    def finish(s, t):
        size = count >> (t + 1)
        src = sources[s] if t == 0 else buffers[s][t - 1]
        dst = buffers[s][t]
        flights[s].wait()
        first = bit_of(all_orders[s][t]) * size

        @pl.loop(0, size)
        def _(i):
            dst[i] = dst[i] + src[first + i]

    slot = slot_of(index, all_orders[streams])

    def spread(u):
        region = pl.ds(slot // 2**u * 2**u, 2**u)
        flights[streams] = copy(
            total.at[region], total.at[region], streams, bits + u,
            all_orders[streams][bits - 1 - u],
        )

    def advance(t):
        if t < bits:
            finish(streams, t)
            if t + 1 < bits:
                begin(streams, t + 1)
            else:
                total[slot] = buffers[streams][t][0]
                spread(0)
        else:
            flights[streams].wait()
            if t + 1 < 2 * bits:
                spread(t + 1 - bits)

    def piece(s):
        high = 4 * LANES

        @pl.loop(0, channels // high)
        def _(m):
            at = pl.ds(pl.multiple_of(m * high, high), high)
            part = jnp.dot(
                ft[at, :],
                cols[:, s * part_width : (s + 1) * part_width],
                preferred_element_type=F32,
            )
            for q in range(4):
                weight = w_ref[4 * m + q]
                block = part[q * LANES : (q + 1) * LANES]
                one = block.astype(BF16)
                left = block - one.astype(F32)
                two = left.astype(BF16)
                three = (left - two.astype(F32)).astype(BF16)
                result = sum(
                    lax.dot_general(
                        weight, x, (((0,), (0,)), ((), ())), preferred_element_type=F32
                    )
                    for x in (one, two, three)
                )
                for j in range(LANES // per):
                    chunk = (4 * m + q) * (LANES // per) + j
                    pieces[s, slot_of(chunk, all_orders[s])] = result[j * per : (j + 1) * per]

    step = 2 * LANES

    def back_part(n):
        at = pl.ds(pl.multiple_of(n * step, step), step)
        grad = jnp.dot(cols[...], k_ref[:, at], preferred_element_type=F32)
        back[:, at] = grad
        summed = jnp.sum(jnp.where(valid, grad, 0.0), axis=0, keepdims=True)
        low = grad.astype(BF16)
        raw = jnp.dot(ft[at, :], low, preferred_element_type=F32)
        fsum = jnp.dot(ones, fp[:, at], preferred_element_type=F32)
        for q in range(2):
            block = raw[q * LANES : (q + 1) * LANES, q * LANES : (q + 1) * LANES]
            where = pl.multiple_of((2 * n + q) * half, half)
            flat[pl.ds(where, half), :] = jnp.where(low_lane, block[:half], block[half:])
            flat[pl.ds(base + 2 * n + q, 1), :] = summed[:, q * LANES : (q + 1) * LANES]
            flat[pl.ds(base + blocks + 2 * n + q, 1), :] = fsum[:1, q * LANES : (q + 1) * LANES]

    def pack_sums():
        colsum = jnp.dot(ones, cols[...], preferred_element_type=F32)
        for q in range(3 * taps // LANES):
            flat[pl.ds(base + 2 * blocks + q, 1), :] = colsum[:1, q * LANES : (q + 1) * LANES]

        @pl.loop(0, count)
        def _(i):
            small[i] = flat[pl.ds(pl.multiple_of(i * rp, 8), rp), :]

    pl.semaphore_wait(barrier, bits)
    for s in range(streams):
        piece(s)
        begin(s, 0)
        if s > 0:
            finish(s - 1, 0)
            begin(s - 1, 1)
    finish(streams - 1, 0)
    begin(streams - 1, 1)
    k_copy.wait()
    turns = channels // step
    pl.loop(0, turns // 2)(back_part)
    for s in range(streams // 2):
        finish(s, 1)
        begin(s, 2)
    pl.loop(turns // 2, turns)(back_part)
    pack_sums()
    begin(streams, 0)
    done = 0
    for t in (1, 2):
        for s in range(streams):
            if t == 2 or s >= streams // 2:
                finish(s, t)
                begin(s, t + 1)
                if done < 2 * bits:
                    advance(done)
                    done += 1
    while done < 2 * bits:
        advance(done)
        done += 1

    @pl.loop(0, count)
    def _(i):
        flat[pl.ds(pl.multiple_of(i * rp, 8), rp), :] = total[i]

    def across(line):
        return jnp.broadcast_to(line, (LANES, LANES)).T

    side = lax.broadcasted_iota(jnp.int32, (LANES, LANES), 0) < half
    other = lax.broadcasted_iota(jnp.int32, (LANES, LANES), 1) < half
    inside = side == other

    @pl.loop(0, blocks)
    def _(k):
        packed = flat[pl.ds(pl.multiple_of(k * half, half), half), :]
        mean = flat[pl.ds(base + blocks + k, 1), :] / pixel_total
        summed = flat[pl.ds(base + k, 1), :]
        raw = jnp.concatenate([packed, packed], axis=0)
        cov = jnp.where(inside, raw - across(mean) * summed, 0.0)
        v = v_ref[k]
        scale = sv_ref[0, pl.ds(k, 1), :]
        root = sv_ref[1, pl.ds(k, 1), :]
        turned = lax.dot_general(
            v, cov, (((0,), (0,)), ((), ())), precision=highest, preferred_element_type=F32
        )
        rotated = jnp.dot(turned, v, precision=highest, preferred_element_type=F32)
        symmetric = 0.5 * (rotated + rotated.T)
        factor = -(across(scale) * scale) / (across(root) + root)
        inner = jnp.where(inside, symmetric * factor, 0.0)
        outer = jnp.dot(v, inner, precision=highest, preferred_element_type=F32)
        sigma = lax.dot_general(
            outer, v, (((1,), (1,)), ((), ())), precision=highest, preferred_element_type=F32
        )
        s_ref[k] = (2.0 / pixel_total * sigma).astype(BF16)

    def final_part(b):
        here = pl.ds(pl.multiple_of(b * image_rows, 16), image_rows)
        for k in range(blocks):
            at = slice(k * LANES, (k + 1) * LANES)
            mean = flat[base + blocks + k : base + blocks + k + 1, :] / pixel_total
            shift = flat[base + k : base + k + 1, :] / pixel_total
            shifted = (back[here, at] - shift).astype(BF16)
            centered = (fp[here, at].astype(F32) - mean).astype(BF16)
            out = jnp.dot(shifted, w_ref[k], preferred_element_type=F32) + jnp.dot(
                centered, s_ref[k], preferred_element_type=F32
            )
            o_ref[b, :, :, at] = out.astype(BF16).reshape(height, wide, LANES)[:, :width]

    pl.loop(0, images // 2)(final_part)
    for s in range(streams):
        finish(s, 3)
        if bits > 4:
            begin(s, 4)
    pl.loop(images // 2, images)(final_part)
    for t in range(4, bits):
        for s in range(streams):
            finish(s, t)
            if t + 1 < bits:
                begin(s, t + 1)

    mine = index * per // LANES
    mean = flat[pl.ds(base + blocks + mine, 1), :] / pixel_total
    whitened = jnp.dot(
        jnp.broadcast_to(mean, (8, LANES)), w_ref[mine].astype(F32),
        precision=highest, preferred_element_type=F32,
    )
    column[...] = across(whitened[:1])
    mean_part = column[pl.ds(pl.multiple_of(index * per % LANES, per), per), :]
    for s in range(streams):
        for q in range(part_width // LANES):
            at = s * (part_width // LANES) + q
            line = flat[base + 2 * blocks + at : base + 2 * blocks + at + 1, :]
            share_ref[:, at * LANES : (at + 1) * LANES] = (
                buffers[s][bits - 1][0, :, q * LANES : (q + 1) * LANES] - mean_part * line
            )


def pair_blocks(blocks):
    groups, size = blocks.shape[:2]
    pairs = blocks.reshape(groups // 2, 2, size, size)
    zero = jnp.zeros((groups // 2, size, size), blocks.dtype)
    top = jnp.concatenate([pairs[:, 0], zero], axis=2)
    bottom = jnp.concatenate([zero, pairs[:, 1]], axis=2)
    return jnp.concatenate([top, bottom], axis=1)


def general_local(shape, features, grads, kernel, vectors, values):
    images, height, width, channels = features.shape
    outputs = grads.shape[3]
    groups, group_size = values.shape
    devices = shape[0] * shape[1]
    bits = devices.bit_length() - 1
    orders = bit_orders(bits)
    per = channels // devices
    taps = 3 * outputs
    wide = round_up(width, 16)
    rows = images * height * wide
    kp = round_up(rows + 1, LANES)
    blocks = channels // LANES
    pixel_total = 1.0 * images * height * width * devices
    small_rows = channels // 2 + 2 * blocks + 3 * taps // LANES
    rp = round_up(-(-small_rows // devices), 8)

    streams = 6
    part_width = 3 * taps // streams
    lines = jnp.stack([lax.rsqrt(values), jnp.sqrt(values)]).reshape(2, blocks, LANES)
    vmem = pl.BlockSpec(memory_space=pltpu.VMEM)
    scratch = []
    for _ in range(streams):
        scratch += [pltpu.VMEM((devices >> (t + 1), per, part_width), F32) for t in range(bits)]
    scratch += [pltpu.VMEM((devices >> (t + 1), rp, LANES), F32) for t in range(bits)]
    sizes = (
        shape[0], shape[1], images, height, width, wide, channels, outputs, per, orders,
        streams, pixel_total,
    )
    input_grad, share = pl.pallas_call(
        functools.partial(general_kernel, sizes),
        out_shape=(
            jax.ShapeDtypeStruct(features.shape, BF16),
            jax.ShapeDtypeStruct((per, 3 * taps), F32),
        ),
        in_specs=[vmem, vmem, pl.BlockSpec(memory_space=pl.ANY), vmem, vmem],
        out_specs=(vmem, vmem),
        scratch_shapes=[
            pltpu.VMEM((kp, channels), BF16),
            pltpu.VMEM((channels, kp), BF16),
            pltpu.VMEM((kp, 3 * taps), BF16),
            pltpu.VMEM((height + 2, wide + 8, outputs), F32),
            pltpu.VMEM((3 * taps, channels), BF16),
            pltpu.VMEM((kp, channels), F32),
            pltpu.VMEM((blocks, LANES, LANES), BF16),
            pltpu.VMEM((blocks, LANES, LANES), BF16),
            pltpu.VMEM((devices * rp, LANES), F32),
            pltpu.VMEM((devices, rp, LANES), F32),
            pltpu.VMEM((devices, rp, LANES), F32),
            pltpu.VMEM((LANES, LANES), F32),
            pltpu.VMEM((streams, devices, per, part_width), F32),
            pltpu.SemaphoreType.DMA,
            pltpu.SemaphoreType.DMA((streams + 1, 2 * bits)),
            pltpu.SemaphoreType.DMA((streams + 1, 2 * bits)),
        ]
        + scratch,
        compiler_params=pltpu.CompilerParams(
            collective_id=0, has_side_effects=True, vmem_limit_bytes=VMEM_LIMIT
        ),
        name="step",
    )(features, grads, kernel.reshape(3 * taps, channels), pair_blocks(vectors), lines)
    return (input_grad, share.reshape(per, 3, 3, outputs))


PAIR, SHALLOW = 2, 2


def plan_kernel(
    sizes, f_ref, g_ref, k_hbm, v_ref, val_ref, o_ref, share_ref,
    fp, ft, cols, gpad, k_ref, back, w_ref, own_ref, s_ref, means,
    parts, swap, near1, near2, zsum, zin, zfar, early_in, early_far, early1, early2,
    total, mixed, mixed_in, stat, stat_in, stat_far, known, table,
    k_sem, send_sem, recv_sem
):
    (images, height, width, wide, channels, outputs, group, depth, pixel_total) = sizes
    rows = images * height * wide
    kp = fp.shape[0]
    groups = channels // group
    blocks = channels // LANES
    tiles = 9
    taps = 3 * outputs
    quarter = group // 2
    plane = groups // depth
    image_rows = height * wide
    packed = quarter // 2

    batch = lax.axis_index("batch")
    row = lax.axis_index("rows")
    core = row % PAIR
    x = row // PAIR
    y = batch % SHALLOW
    z = batch // SHALLOW
    chip = (z * SHALLOW + y) * SHALLOW + x
    znear = z + 1 - 2 * (z % 2)
    zother = depth - 1 - z
    outer = (z == 0) | (z == depth - 1)
    inner = (z > 0) & (z < depth - 1)

    def place(x, y, z, core=core):
        return (z * SHALLOW + y, x * PAIR + core)

    partner = place(x, y, z, 1 - core)
    xside = place(1 - x, y, z)
    yside = place(x, 1 - y, z)

    def peer(k):
        px = 1 - x if k % 2 else x
        py = 1 - y if k // 2 % 2 else y
        low = 1 - z % 2 if k // 4 % 2 else z % 2
        high = 1 - z // 2 if k // 8 % 2 else z // 2
        pz = high * 2 + low
        return px, py, pz

    barrier = pltpu.get_barrier_semaphore()
    greet = [partner] + [place(*peer(k)) for k in range(1, groups)]
    for other in greet:
        pl.semaphore_signal(
            barrier, inc=1, device_id=other, device_id_type=pl.DeviceIdType.MESH
        )
    k_copy = pltpu.make_async_copy(k_hbm, k_ref, k_sem)
    k_copy.start()

    sems = {}

    def copy(key, src, dst, device, landing=None):
        at = sems.setdefault(key, len(sems))
        to = at if landing is None else sems.setdefault(landing, len(sems))
        return pltpu.make_async_remote_copy(
            src_ref=src, dst_ref=dst, send_sem=send_sem.at[at], recv_sem=recv_sem.at[to],
            device_id=device, device_id_type=pl.DeviceIdType.MESH,
        )

    flights = {}

    def send(key, src, dst, device):
        flights[key] = copy(key, src, dst, device)
        flights[key].start()

    def arrive(key):
        flights.pop(key).wait()

    fp[pl.ds(rows, kp - rows), :] = jnp.zeros((kp - rows, channels), BF16)
    cols[pl.ds(rows, kp - rows), :] = jnp.zeros((kp - rows, 3 * taps), BF16)
    gpad[...] = jnp.zeros(gpad.shape, F32)

    @pl.loop(0, images)
    def _(b):
        gpad[pl.ds(1, height), pl.ds(1, width), :] = g_ref[b].astype(F32)
        for h in range(height):
            at = pl.multiple_of((b * height + h) * wide, 16)
            fp[pl.ds(at, wide), :] = jnp.zeros((wide, channels), BF16)
            fp[pl.ds(at, width), :] = f_ref[b, h]
        at = pl.multiple_of(b * image_rows, 16)
        for c in range(3):
            shifted = gpad[:, 2 - c : 2 - c + wide, :].astype(BF16)
            for a in range(3):
                first = a * taps + c * outputs
                cols[pl.ds(at, image_rows), first : first + outputs] = shifted[
                    2 - a : 2 - a + height
                ].reshape(image_rows, outputs)

    @pl.loop(0, blocks)
    def _(k):
        at = pl.ds(pl.multiple_of(k * LANES, LANES), LANES)
        ft[at, :] = fp[:, at].T

    position = lax.broadcasted_iota(jnp.int32, (kp, 1), 0)
    valid = (position % wide < width) & (position < rows)
    lane = lax.broadcasted_iota(jnp.int32, (16, kp), 1)
    ft[pl.ds(channels, 16), :] = jnp.where(
        (lane % wide < width) & (lane < rows), 1.0, 0.0
    ).astype(BF16)
    stat[:, :, pl.ds(packed, 8), :] = jnp.zeros((PAIR, groups, 8, LANES), F32)

    first_plane = [0, 2, 4, 5, 6, 7, 8]
    first_depth = [1, 3]

    def slot(t, half, g):
        gz, gy, gx = g // 4, g // 2 % 2, g % 2
        first, second = (gx, gy) if half == 0 else (gy, gx)
        if t in first_depth:
            return gz * 4 + first * 2 + second
        return first * 8 + second * 4 + gz

    def tile(t):
        high = channels // 2
        for m in range(2):
            extra = 16 if m == 1 else 0
            part = jnp.dot(
                ft[m * high : (m + 1) * high + extra, :],
                cols[:, t * outputs : (t + 1) * outputs],
                preferred_element_type=F32,
            )
            for q in range(groups // 2):
                g = m * (groups // 2) + q
                for half in range(2):
                    lines = slice(q * group + half * quarter, q * group + (half + 1) * quarter)
                    for c in range(PAIR):
                        parts[t, c, half, slot(t, half, g)] = part[
                            lines, c * LANES : (c + 1) * LANES
                        ]
            if m == 1:
                for c in range(PAIR):
                    stat[c, t, packed + 1 : packed + 2, :] = part[
                        high : high + 1, c * LANES : (c + 1) * LANES
                    ]
        send(("swap", t), parts.at[t, 1 - core], swap.at[t], partner)

    def add(dst, src, dst_first, count, src_first=0):
        @pl.loop(0, count)
        def _(i):
            dst[dst_first + i] = dst[dst_first + i] + src[src_first + i]

    def mine(t, half):
        return parts.at[t, core, half]

    firsts = [(x, y), (y, x)]
    sides = [(xside, yside), (yside, xside)]

    def swapped(t):
        arrive(("swap", t))
        for half in range(2):
            add(mine(t, half), swap.at[t, half], 0, groups)

    def plane1(t):
        for half in range(2):
            send(
                ("p1", t, half),
                mine(t, half).at[pl.ds((1 - firsts[half][0]) * 8, 8)],
                near1.at[t, half], sides[half][0],
            )

    def plane2(t):
        for half in range(2):
            arrive(("p1", t, half))
            f, s = firsts[half]
            add(mine(t, half), near1.at[t, half], f * 8 + (1 - s) * 4, 4, (1 - s) * 4)
            send(
                ("p2", t, half),
                mine(t, half).at[pl.ds(f * 8 + (1 - s) * 4, 4)],
                near2.at[t, half], sides[half][1],
            )
        for half in range(2):
            f, s = firsts[half]
            add(mine(t, half), near1.at[t, half], f * 8 + s * 4, 4, s * 4)

    def depth1(t):
        for half in range(2):
            arrive(("p2", t, half))
            f, s = firsts[half]
            src = mine(t, half)
            for j in range(depth):
                zsum[t, j, pl.ds(half * quarter, quarter)] = (
                    src[f * 8 + s * 4 + j] + near2[t, half, j]
                )
        key = ("z1", t)

        @pl.when(outer)
        def _():
            copy(
                key, zsum.at[t, pl.ds((depth - 1 - z) // 3, 3)], zin.at[t], place(x, y, znear)
            ).start()

        @pl.when(inner)
        def _():
            copy(
                key, zsum.at[t, pl.ds(znear, 1)], zin.at[t, pl.ds(0, 1)], place(x, y, znear)
            ).start()

    def depth2(t):
        key = ("z1", t)

        @pl.when(outer)
        def _():
            near = place(x, y, znear)
            copy(key, zsum.at[t, pl.ds((depth - 1 - z) // 3, 3)], zin.at[t], near).wait_send()
            copy(key, zsum.at[t, pl.ds(0, 1)], zin.at[t, pl.ds(0, 1)], near).wait_recv()
            zsum[t, z] = zsum[t, z] + zin[t, 0]

        @pl.when(inner)
        def _():
            near = place(x, y, znear)
            copy(key, zsum.at[t, pl.ds(znear, 1)], zin.at[t, pl.ds(0, 1)], near).wait_send()
            copy(key, zsum.at[t, pl.ds(0, 3)], zin.at[t], near).wait_recv()
            for j in range(3):
                zsum[t, 2 - z + j] = zsum[t, 2 - z + j] + zin[t, j]
            copy(
                ("z2", t), zsum.at[t, pl.ds(zother, 1)], zfar.at[t], place(x, y, zother)
            ).start()
            zfin = 3 * (2 - z)
            copy(
                ("z3", t), zsum.at[t, pl.ds(zfin, 1)], zfar.at[t], place(x, y, zfin), ("z2", t)
            ).start()

    def depth3(t):
        @pl.when(inner)
        def _():
            copy(
                ("z2", t), zsum.at[t, pl.ds(zother, 1)], zfar.at[t], place(x, y, zother)
            ).wait_send()
            zfin = 3 * (2 - z)
            copy(
                ("z3", t), zsum.at[t, pl.ds(zfin, 1)], zfar.at[t], place(x, y, zfin), ("z2", t)
            ).wait_send()

        copy(
            ("z2", t), zsum.at[t, pl.ds(0, 1)], zfar.at[t], place(x, y, zother)
        ).wait_recv()
        total[t] = zsum[t, z] + zfar[t, 0]

    def early1_start(t, half):
        e = first_depth.index(t)
        key = ("e1", t, half)
        src = mine(t, half)

        @pl.when(outer)
        def _():
            copy(
                key, src.at[pl.ds((depth - 1 - z) // 3 * 4, 12)], early_in.at[e, half],
                place(x, y, znear),
            ).start()

        @pl.when(inner)
        def _():
            copy(
                key, src.at[pl.ds(znear * 4, 4)], early_in.at[e, half, pl.ds(0, 4)],
                place(x, y, znear),
            ).start()

    def early2_start(t, half):
        e = first_depth.index(t)
        key = ("e1", t, half)
        src = mine(t, half)
        buf = early_in.at[e, half]
        far = early_far.at[e, half]

        @pl.when(outer)
        def _():
            near = place(x, y, znear)
            copy(key, src.at[pl.ds((depth - 1 - z) // 3 * 4, 12)], buf, near).wait_send()
            copy(key, src.at[pl.ds(0, 4)], buf.at[pl.ds(0, 4)], near).wait_recv()
            add(src, buf, z * 4, 4)

        @pl.when(inner)
        def _():
            near = place(x, y, znear)
            copy(key, src.at[pl.ds(znear * 4, 4)], buf.at[pl.ds(0, 4)], near).wait_send()
            copy(key, src.at[pl.ds(0, 12)], buf, near).wait_recv()
            add(src, buf, (2 - z) * 4, 12)
            copy(
                ("e2", t, half), src.at[pl.ds(zother * 4, 4)], far, place(x, y, zother)
            ).start()
            zfin = 3 * (2 - z)
            copy(
                ("e3", t, half), src.at[pl.ds(zfin * 4, 4)], far, place(x, y, zfin),
                ("e2", t, half),
            ).start()

    def early3_start(t, half):
        e = first_depth.index(t)
        src = mine(t, half)
        far = early_far.at[e, half]

        @pl.when(inner)
        def _():
            copy(
                ("e2", t, half), src.at[pl.ds(zother * 4, 4)], far, place(x, y, zother)
            ).wait_send()
            zfin = 3 * (2 - z)
            copy(
                ("e3", t, half), src.at[pl.ds(zfin * 4, 4)], far, place(x, y, zfin),
                ("e2", t, half),
            ).wait_send()

        copy(("e2", t, half), src.at[pl.ds(0, 4)], far, place(x, y, zother)).wait_recv()
        add(src, far, z * 4, 4)
        send(
            ("e4", t, half),
            src.at[pl.ds(z * 4 + (1 - firsts[half][0]) * 2, 2)],
            early1.at[e, half], sides[half][0],
        )

    def early4_start(t, half):
        e = first_depth.index(t)
        arrive(("e4", t, half))
        f, s = firsts[half]
        src = mine(t, half)
        add(src, early1.at[e, half], z * 4 + f * 2, 2)
        send(
            ("e5", t, half),
            src.at[pl.ds(z * 4 + f * 2 + (1 - s), 1)],
            early2.at[e, half], sides[half][1],
        )

    def early5(t, half):
        e = first_depth.index(t)
        arrive(("e5", t, half))
        f, s = firsts[half]
        src = mine(t, half)
        total[t, pl.ds(half * quarter, quarter)] = (
            src[z * 4 + f * 2 + s] + early2[e, half, 0]
        )

    step = 2 * LANES
    half_rows = kp // 2
    low_lane = lax.broadcasted_iota(jnp.int32, (quarter, LANES), 1) < LANES // 2
    low_line = lax.broadcasted_iota(jnp.int32, (8, LANES), 1) < LANES // 2

    def turn(a):
        return pltpu.roll(a, LANES // 2, 1)

    def back_part(n, r):
        at = slice(n * step, (n + 1) * step)
        here = slice(r * half_rows, (r + 1) * half_rows)
        back[here, at] = jnp.dot(cols[here, :], k_ref[:, at], preferred_element_type=F32)

    def cov_part(n):
        at = slice(n * step, (n + 1) * step)
        grad = back[:, at]
        summed = jnp.broadcast_to(
            jnp.sum(jnp.where(valid, grad, 0.0), axis=0, keepdims=True), (8, step)
        )
        raw = jnp.dot(ft[at, :], grad.astype(BF16), preferred_element_type=F32)
        fsum = jnp.dot(ft[channels : channels + 16, :], fp[:, at], preferred_element_type=F32)[:8]
        for q in range(2):
            wide_at = slice(q * LANES, (q + 1) * LANES)
            block = raw[wide_at, wide_at]
            bs, fs = summed[:, wide_at], fsum[:, wide_at]
            g = (2 * n + q) * 2
            pieces = [block[i * quarter : (i + 1) * quarter] for i in range(4)]
            lower = jnp.where(low_lane, pieces[0], turn(pieces[1]))
            upper = jnp.where(low_lane, turn(pieces[2]), pieces[3])
            for c in range(PAIR):
                stat[c, g, :packed] = lower[c * packed : (c + 1) * packed]
                stat[c, g + 1, :packed] = upper[c * packed : (c + 1) * packed]
            stat[0, g, packed : packed + 1] = jnp.where(low_line, fs, turn(bs))[:1]
            stat[0, g + 1, packed : packed + 1] = jnp.where(low_line, turn(fs), bs)[:1]

    def stat1():
        send("s1", stat.at[1 - core], stat_in, partner)

    def stat2():
        arrive("s1")
        src = stat.at[core]
        add(src, stat_in, 0, groups)
        for k in range(1, groups):
            px, py, pz = peer(k)
            send(
                ("s2", k), src.at[(pz * SHALLOW + py) * SHALLOW + px], stat_far.at[k],
                place(px, py, pz),
            )

    def stat3():
        summed = stat[core, chip]
        for k in range(1, groups):
            arrive(("s2", k))
            summed = summed + stat_far[k]
        known[core] = summed
        send("s3", known.at[core], known.at[core], partner)

    def across(line):
        return jnp.broadcast_to(line, (LANES, LANES)).T[:group, :group]

    def hdot(a, b, dims):
        return lax.dot_general(
            a, b, (dims, ((), ())), precision=highest, preferred_element_type=F32
        )

    def stat4():
        arrive("s3")
        lines = jnp.concatenate([known[0, :packed], known[1, :packed]], axis=0)
        raw = jnp.concatenate([lines, turn(lines)], axis=0)[:, :group]
        both = jnp.broadcast_to(known[0, packed : packed + 1], (8, LANES))
        mean = both[:1] / pixel_total
        summed = turn(both)[:1, :group]
        cov = raw - across(mean) * summed
        v = v_ref[chip]
        vals = jnp.concatenate(
            [val_ref[pl.ds(chip, 1), :], jnp.ones((1, LANES - group), F32)], axis=1
        )
        scale = lax.rsqrt(vals)
        root = jnp.sqrt(vals)
        turned = hdot(v, cov, ((0,), (0,)))
        rotated = hdot(turned, v, ((1,), (0,)))
        symmetric = 0.5 * (rotated + rotated.T)
        factor = -(across(scale) * scale[:, :group]) / (across(root) + root[:, :group])
        inside = hdot(v, symmetric * factor, ((1,), (0,)))
        sigma = 2.0 / pixel_total * hdot(inside, v, ((1,), (1,)))
        own_ref[...] = hdot(v * scale[:, :group], v, ((1,), (1,))).astype(BF16)
        sigma = jnp.concatenate([sigma, jnp.zeros((group, LANES - group), F32)], axis=1)
        folded = jnp.where(low_lane, sigma[:quarter], turn(sigma[quarter:]))
        table[core, chip, :packed] = jnp.where(core == 0, folded[:packed], folded[packed:])
        table[core, chip, packed:] = known[core, packed:]
        table[core, chip, packed : packed + 1] = known[0, packed : packed + 1]
        src = table.at[core, chip]
        for k in range(1, groups):
            send(("s4", k), src, src, place(*peer(k)))

    def stat5():
        for k in range(1, groups):
            arrive(("s4", k))
        send("s5", table.at[core], table.at[core], partner)

    def stat6():
        arrive("s5")
        for k in range(blocks):
            folded = [
                jnp.concatenate([table[0, 2 * k + q, :packed], table[1, 2 * k + q, :packed]], axis=0)
                for q in range(2)
            ]
            s_ref[k] = jnp.concatenate(
                [
                    jnp.where(low_lane, folded[0], 0.0),
                    jnp.where(low_lane, turn(folded[0]), 0.0),
                    jnp.where(low_lane, 0.0, turn(folded[1])),
                    jnp.where(low_lane, 0.0, folded[1]),
                ],
                axis=0,
            ).astype(BF16)
            sums = [
                jnp.broadcast_to(table[0, 2 * k + q, packed : packed + 1], (8, LANES))
                for q in range(2)
            ]
            means[0, k] = jnp.where(low_line, sums[0], turn(sums[1])) / pixel_total
            means[1, k] = jnp.where(low_line, turn(sums[0]), sums[1]) / pixel_total

    def whiten_part(k):
        zero = jnp.zeros((group, LANES - group), F32)
        for q in range(2):
            g = 2 * k + q
            v = v_ref[g]
            scaled = v * lax.rsqrt(val_ref[g : g + 1, :])
            w = jnp.concatenate([hdot(scaled, v, ((1,), (1,))), zero], axis=1)
            if q == 1:
                w = turn(w)
            w_ref[k, q * group : (q + 1) * group, :] = w.astype(BF16)

    def final_part(b):
        here = pl.ds(pl.multiple_of(b * image_rows, 16), image_rows)
        for k in range(blocks):
            at = slice(k * LANES, (k + 1) * LANES)
            shifted = (back[here, at] - means[1, k, :1]).astype(BF16)
            centered = (fp[here, at].astype(F32) - means[0, k, :1]).astype(BF16)
            out = jnp.dot(shifted, w_ref[k], preferred_element_type=F32) + jnp.dot(
                centered, s_ref[k], preferred_element_type=F32
            )
            o_ref[b, :, :, at] = out.astype(BF16).reshape(height, wide, LANES)[:, :width]

    def whitened(t):
        both = known[0, packed : packed + 1] / pixel_total
        mean = jnp.broadcast_to(both, (LANES, LANES)).T[:group]
        block = total[t] - mean * table[core, t, packed + 1 : packed + 2]
        one = block.astype(BF16)
        left = block - one.astype(F32)
        two = left.astype(BF16)
        three = (left - two.astype(F32)).astype(BF16)
        weight = own_ref[...]
        mixed[t] = sum(
            lax.dot_general(weight, a, (((0,), (0,)), ((), ())), preferred_element_type=F32)
            for a in (one, two, three)
        )
        send(("m", t), mixed.at[t, pl.ds((1 - core) * quarter, quarter)], mixed_in.at[t], partner)
        here = pl.ds(pl.multiple_of(core * LANES, LANES), LANES)
        share_ref[t, :, here] = mixed[t, pl.ds(core * quarter, quarter)]

    def finished(t):
        arrive(("m", t))
        there = pl.ds(pl.multiple_of((1 - core) * LANES, LANES), LANES)
        share_ref[t, :, there] = mixed_in[t]

    p = first_plane
    e = first_depth
    early = [(t, half) for t in e for half in range(2)]
    pl.semaphore_wait(barrier, len(greet))
    tile(p[0])
    tile(e[0])
    tile(p[1])
    swapped(p[0])
    plane1(p[0])
    tile(e[1])
    swapped(e[0])
    early1_start(*early[0])
    early1_start(*early[1])
    tile(p[2])
    swapped(p[1])
    plane1(p[1])
    tile(p[3])
    swapped(e[1])
    early1_start(*early[2])
    early1_start(*early[3])
    tile(p[4])
    swapped(p[2])
    plane1(p[2])
    tile(p[5])
    swapped(p[3])
    plane2(p[0])
    plane1(p[3])
    tile(p[6])
    swapped(p[4])
    k_copy.wait()
    back_part(0, 0)
    swapped(p[5])
    back_part(0, 1)
    early2_start(*early[0])
    plane2(p[1])
    plane1(p[4])
    cov_part(0)
    swapped(p[6])
    back_part(1, 0)
    back_part(1, 1)
    plane2(p[2])
    plane1(p[5])
    early2_start(*early[1])
    cov_part(1)
    depth1(p[0])
    back_part(2, 0)
    early3_start(*early[0])
    back_part(2, 1)
    plane2(p[3])
    plane1(p[6])
    cov_part(2)
    early2_start(*early[2])
    back_part(3, 0)
    depth1(p[1])
    back_part(3, 1)
    plane2(p[4])
    cov_part(3)
    stat1()
    early3_start(*early[1])
    whiten_part(0)
    whiten_part(1)
    stat2()
    early2_start(*early[3])
    depth1(p[2])
    for k in range(2, blocks):
        whiten_part(k)
    plane2(p[5])
    early4_start(*early[0])
    early4_start(*early[1])
    depth2(p[0])
    stat3()
    early3_start(*early[2])
    stat4()
    depth1(p[3])
    depth2(p[1])
    plane2(p[6])
    early5(*early[0])
    early5(*early[1])
    early3_start(*early[3])
    depth2(p[2])
    depth1(p[4])
    depth3(p[0])
    depth3(p[1])
    stat5()
    early4_start(*early[2])
    early4_start(*early[3])
    depth2(p[3])
    depth1(p[5])
    stat6()
    depth3(p[2])
    pl.loop(0, images // 3)(final_part)
    depth1(p[6])
    depth2(p[4])
    depth3(p[3])
    pl.loop(images // 3, 2 * images // 3)(final_part)
    early5(*early[2])
    early5(*early[3])
    depth2(p[5])
    depth3(p[4])
    pl.loop(2 * images // 3, images)(final_part)
    for t in (e[0], e[1], p[0], p[1], p[2], p[3], p[4]):
        whitened(t)
    depth2(p[6])
    depth3(p[5])
    whitened(p[5])
    for t in (e[0], e[1], p[0], p[1], p[2], p[3], p[4]):
        finished(t)
    depth3(p[6])
    whitened(p[6])
    finished(p[5])
    finished(p[6])


def plan_local(shape, features, grads, kernel, vectors, values):
    images, height, width, channels = features.shape
    outputs = grads.shape[3]
    groups, group = values.shape
    devices = shape[0] * shape[1]
    depth = shape[0] // SHALLOW
    taps = 3 * outputs
    wide = round_up(width, 16)
    rows = images * height * wide
    kp = round_up(rows + 1, LANES)
    blocks = channels // LANES
    pixel_total = 1.0 * images * height * width * devices
    quarter = group // 2
    stat_rows = quarter // 2 + 8
    sizes = (images, height, width, wide, channels, outputs, group, depth, pixel_total)
    vmem = pl.BlockSpec(memory_space=pltpu.VMEM)
    sem_count = 192
    f32 = [
        (9, PAIR, 2, groups, quarter, LANES),
        (9, 2, groups, quarter, LANES),
        (9, 2, 8, quarter, LANES),
        (9, 2, 4, quarter, LANES),
        (9, depth, group, LANES),
        (9, 3, group, LANES),
        (9, 1, group, LANES),
        (2, 2, 12, quarter, LANES),
        (2, 2, 4, quarter, LANES),
        (2, 2, 2, quarter, LANES),
        (2, 2, 1, quarter, LANES),
        (9, group, LANES),
        (9, group, LANES),
        (9, quarter, LANES),
        (PAIR, groups, stat_rows, LANES),
        (groups, stat_rows, LANES),
        (groups, stat_rows, LANES),
        (PAIR, stat_rows, LANES),
        (PAIR, groups, stat_rows, LANES),
    ]
    input_grad, share = pl.pallas_call(
        functools.partial(plan_kernel, sizes),
        out_shape=(
            jax.ShapeDtypeStruct(features.shape, BF16),
            jax.ShapeDtypeStruct((9, channels // devices, outputs), F32),
        ),
        in_specs=[vmem, vmem, pl.BlockSpec(memory_space=pl.ANY), vmem, vmem],
        out_specs=(vmem, vmem),
        scratch_shapes=[
            pltpu.VMEM((kp, channels), BF16),
            pltpu.VMEM((channels + 16, kp), BF16),
            pltpu.VMEM((kp, 3 * taps), BF16),
            pltpu.VMEM((height + 2, wide + 8, outputs), F32),
            pltpu.VMEM((3 * taps, channels), BF16),
            pltpu.VMEM((kp, channels), F32),
            pltpu.VMEM((blocks, LANES, LANES), BF16),
            pltpu.VMEM((group, group), BF16),
            pltpu.VMEM((blocks, LANES, LANES), BF16),
            pltpu.VMEM((2, blocks, 8, LANES), F32),
        ]
        + [pltpu.VMEM(s, F32) for s in f32]
        + [
            pltpu.SemaphoreType.DMA,
            pltpu.SemaphoreType.DMA((sem_count,)),
            pltpu.SemaphoreType.DMA((sem_count,)),
        ],
        compiler_params=pltpu.CompilerParams(
            collective_id=0, has_side_effects=True, vmem_limit_bytes=VMEM_LIMIT
        ),
        name="step",
    )(features, grads, kernel.reshape(3 * taps, channels), vectors, values)
    per = channels // devices
    return (input_grad, share.reshape(3, 3, per, outputs).transpose(2, 0, 1, 3))


def solution(mesh):
    shape = (mesh.shape["batch"], mesh.shape["rows"])
    split = P(("batch", "rows"), None, None, None)

    def local(features, grads, kernel, vectors, values):
        groups, group = values.shape
        fits = (
            shape == (SHALLOW * 4, PAIR * SHALLOW)
            and groups * PAIR == shape[0] * shape[1]
            and group * 2 == LANES
            and grads.shape[3] == PAIR * LANES
            and features.shape[0] % 3 == 0
        )
        body = plan_local if fits else general_local
        return body(shape, features, grads, kernel, vectors, values)

    return jax.shard_map(
        local,
        mesh=mesh,
        in_specs=(split, split, P(), P(), P()),
        out_specs=(split, split),
        check_vma=False,
    )
```

```python
import functools
import jax
import jax.numpy as jnp
from jax import lax
from jax.experimental import pallas as pl
from jax.experimental.pallas import tpu as pltpu
from jax.sharding import PartitionSpec as P

highest = lax.Precision.HIGHEST
F32, BF16 = jnp.float32, jnp.bfloat16
LANES = 128
VMEM_LIMIT = 63 * 1024 * 1024


def round_up(n, m):
    return (n + m - 1) // m * m


def bit_orders(bits):
    rest = list(range(1, bits))
    first = [0] + rest
    second = [0] + rest[1:2] + rest[:1] + rest[2:]
    third = [0] + rest[2:3] + rest[:2] + rest[3:]
    return [first, second, third]


def slot_of(index, order):
    slot = 0
    count = len(order)
    for step, bit in enumerate(order):
        slot = slot + (index // 2**bit) % 2 * 2 ** (count - 1 - step)
    return slot


def general_kernel(
    sizes, f_ref, g_ref, k_hbm, v_ref, sv_ref, o_ref, share_ref,
    fp, ft, cols, gpad, k_ref, back, w_ref, s_ref, flat, small, total, column, pieces,
    k_sem, send_sem, recv_sem, *scratch
):
    (nb, nr, images, height, width, wide, channels, outputs, per, orders, streams, pixel_total) = sizes
    rows = images * height * wide
    kp = fp.shape[0]
    blocks = channels // LANES
    taps = 3 * outputs
    part_width = 3 * taps // streams
    bits = len(orders[0])
    count = 2**bits
    rp = small.shape[1]
    half = LANES // 2
    base = channels // 2
    image_rows = height * wide
    batch = lax.axis_index("batch")
    row = lax.axis_index("rows")
    index = batch * nr + row

    def bit_of(bit):
        return (index // 2**bit) % 2

    def partner(bit):
        sign = 1 - 2 * bit_of(bit)
        if 2**bit < nr:
            return (batch, row + sign * 2**bit)
        return (batch + sign * (2**bit // nr), row)

    barrier = pltpu.get_barrier_semaphore()
    for bit in range(bits):
        pl.semaphore_signal(
            barrier, inc=1, device_id=partner(bit), device_id_type=pl.DeviceIdType.MESH
        )
    k_copy = pltpu.make_async_copy(k_hbm, k_ref, k_sem)
    k_copy.start()

    fp[pl.ds(rows, kp - rows), :] = jnp.zeros((kp - rows, channels), BF16)
    cols[pl.ds(rows, kp - rows), :] = jnp.zeros((kp - rows, 3 * taps), BF16)
    gpad[...] = jnp.zeros(gpad.shape, F32)

    @pl.loop(0, images)
    def _(b):
        gpad[pl.ds(1, height), pl.ds(1, width), :] = g_ref[b].astype(F32)
        for h in range(height):
            at = pl.multiple_of((b * height + h) * wide, 16)
            fp[pl.ds(at, wide), :] = jnp.zeros((wide, channels), BF16)
            fp[pl.ds(at, width), :] = f_ref[b, h]
        at = pl.multiple_of(b * image_rows, 16)
        for c in range(3):
            shifted = gpad[:, 2 - c : 2 - c + wide, :].astype(BF16)
            for a in range(3):
                first = a * taps + c * outputs
                cols[pl.ds(at, image_rows), first : first + outputs] = shifted[
                    2 - a : 2 - a + height
                ].reshape(image_rows, outputs)

    @pl.loop(0, blocks)
    def _(k):
        at = pl.ds(pl.multiple_of(k * LANES, LANES), LANES)
        ft[at, :] = fp[:, at].T
        v = v_ref[k]
        w_ref[k] = lax.dot_general(
            v * sv_ref[0, pl.ds(k, 1), :], v, (((1,), (1,)), ((), ())),
            precision=highest, preferred_element_type=F32,
        ).astype(BF16)

    position = lax.broadcasted_iota(jnp.int32, (kp, 1), 0)
    valid = (position % wide < width) & (position < rows)
    lane = lax.broadcasted_iota(jnp.int32, (8, kp), 1)
    ones = jnp.where((lane % wide < width) & (lane < rows), 1.0, 0.0).astype(BF16)
    low_lane = lax.broadcasted_iota(jnp.int32, (half, LANES), 1) < half
    flat[pl.ds(base, flat.shape[0] - base), :] = jnp.zeros((flat.shape[0] - base, LANES), F32)

    def copy(src, dst, s, t, bit):
        c = pltpu.make_async_remote_copy(
            src_ref=src,
            dst_ref=dst,
            send_sem=send_sem.at[s, t],
            recv_sem=recv_sem.at[s, t],
            device_id=partner(bit),
            device_id_type=pl.DeviceIdType.MESH,
        )
        c.start()
        return c

    sources = [pieces.at[s] for s in range(streams)] + [small]
    buffers = [[scratch[s * bits + t] for t in range(bits)] for s in range(streams + 1)]
    all_orders = [orders[s % 3] for s in range(streams)] + [orders[0]]
    flights = {}

    def begin(s, t):
        bit = all_orders[s][t]
        size = count >> (t + 1)
        src = sources[s] if t == 0 else buffers[s][t - 1]
        flights[s] = copy(
            src.at[pl.ds((1 - bit_of(bit)) * size, size)], buffers[s][t], s, t, bit
        )

    def finish(s, t):
        size = count >> (t + 1)
        src = sources[s] if t == 0 else buffers[s][t - 1]
        dst = buffers[s][t]
        flights[s].wait()
        first = bit_of(all_orders[s][t]) * size

        @pl.loop(0, size)
        def _(i):
            dst[i] = dst[i] + src[first + i]

    slot = slot_of(index, all_orders[streams])

    def spread(u):
        region = pl.ds(slot // 2**u * 2**u, 2**u)
        flights[streams] = copy(
            total.at[region], total.at[region], streams, bits + u,
            all_orders[streams][bits - 1 - u],
        )

    def advance(t):
        if t < bits:
            finish(streams, t)
            if t + 1 < bits:
                begin(streams, t + 1)
            else:
                total[slot] = buffers[streams][t][0]
                spread(0)
        else:
            flights[streams].wait()
            if t + 1 < 2 * bits:
                spread(t + 1 - bits)

    def piece(s):
        high = 4 * LANES

        @pl.loop(0, channels // high)
        def _(m):
            at = pl.ds(pl.multiple_of(m * high, high), high)
            part = jnp.dot(
                ft[at, :],
                cols[:, s * part_width : (s + 1) * part_width],
                preferred_element_type=F32,
            )
            for q in range(4):
                weight = w_ref[4 * m + q]
                block = part[q * LANES : (q + 1) * LANES]
                one = block.astype(BF16)
                left = block - one.astype(F32)
                two = left.astype(BF16)
                three = (left - two.astype(F32)).astype(BF16)
                result = sum(
                    lax.dot_general(
                        weight, x, (((0,), (0,)), ((), ())), preferred_element_type=F32
                    )
                    for x in (one, two, three)
                )
                for j in range(LANES // per):
                    chunk = (4 * m + q) * (LANES // per) + j
                    pieces[s, slot_of(chunk, all_orders[s])] = result[j * per : (j + 1) * per]

    step = 2 * LANES

    def back_part(n):
        at = pl.ds(pl.multiple_of(n * step, step), step)
        grad = jnp.dot(cols[...], k_ref[:, at], preferred_element_type=F32)
        back[:, at] = grad
        summed = jnp.sum(jnp.where(valid, grad, 0.0), axis=0, keepdims=True)
        low = grad.astype(BF16)
        raw = jnp.dot(ft[at, :], low, preferred_element_type=F32)
        fsum = jnp.dot(ones, fp[:, at], preferred_element_type=F32)
        for q in range(2):
            block = raw[q * LANES : (q + 1) * LANES, q * LANES : (q + 1) * LANES]
            where = pl.multiple_of((2 * n + q) * half, half)
            flat[pl.ds(where, half), :] = jnp.where(low_lane, block[:half], block[half:])
            flat[pl.ds(base + 2 * n + q, 1), :] = summed[:, q * LANES : (q + 1) * LANES]
            flat[pl.ds(base + blocks + 2 * n + q, 1), :] = fsum[:1, q * LANES : (q + 1) * LANES]

    def pack_sums():
        colsum = jnp.dot(ones, cols[...], preferred_element_type=F32)
        for q in range(3 * taps // LANES):
            flat[pl.ds(base + 2 * blocks + q, 1), :] = colsum[:1, q * LANES : (q + 1) * LANES]

        @pl.loop(0, count)
        def _(i):
            small[i] = flat[pl.ds(pl.multiple_of(i * rp, 8), rp), :]

    pl.semaphore_wait(barrier, bits)
    for s in range(streams):
        piece(s)
        begin(s, 0)
        if s > 0:
            finish(s - 1, 0)
            begin(s - 1, 1)
    finish(streams - 1, 0)
    begin(streams - 1, 1)
    k_copy.wait()
    turns = channels // step
    pl.loop(0, turns // 2)(back_part)
    for s in range(streams // 2):
        finish(s, 1)
        begin(s, 2)
    pl.loop(turns // 2, turns)(back_part)
    pack_sums()
    begin(streams, 0)
    done = 0
    for t in (1, 2):
        for s in range(streams):
            if t == 2 or s >= streams // 2:
                finish(s, t)
                begin(s, t + 1)
                if done < 2 * bits:
                    advance(done)
                    done += 1
    while done < 2 * bits:
        advance(done)
        done += 1

    @pl.loop(0, count)
    def _(i):
        flat[pl.ds(pl.multiple_of(i * rp, 8), rp), :] = total[i]

    def across(line):
        return jnp.broadcast_to(line, (LANES, LANES)).T

    side = lax.broadcasted_iota(jnp.int32, (LANES, LANES), 0) < half
    other = lax.broadcasted_iota(jnp.int32, (LANES, LANES), 1) < half
    inside = side == other

    @pl.loop(0, blocks)
    def _(k):
        packed = flat[pl.ds(pl.multiple_of(k * half, half), half), :]
        mean = flat[pl.ds(base + blocks + k, 1), :] / pixel_total
        summed = flat[pl.ds(base + k, 1), :]
        raw = jnp.concatenate([packed, packed], axis=0)
        cov = jnp.where(inside, raw - across(mean) * summed, 0.0)
        v = v_ref[k]
        scale = sv_ref[0, pl.ds(k, 1), :]
        root = sv_ref[1, pl.ds(k, 1), :]
        turned = lax.dot_general(
            v, cov, (((0,), (0,)), ((), ())), precision=highest, preferred_element_type=F32
        )
        rotated = jnp.dot(turned, v, precision=highest, preferred_element_type=F32)
        symmetric = 0.5 * (rotated + rotated.T)
        factor = -(across(scale) * scale) / (across(root) + root)
        inner = jnp.where(inside, symmetric * factor, 0.0)
        outer = jnp.dot(v, inner, precision=highest, preferred_element_type=F32)
        sigma = lax.dot_general(
            outer, v, (((1,), (1,)), ((), ())), precision=highest, preferred_element_type=F32
        )
        s_ref[k] = (2.0 / pixel_total * sigma).astype(BF16)

    def final_part(b):
        here = pl.ds(pl.multiple_of(b * image_rows, 16), image_rows)
        for k in range(blocks):
            at = slice(k * LANES, (k + 1) * LANES)
            mean = flat[base + blocks + k : base + blocks + k + 1, :] / pixel_total
            shift = flat[base + k : base + k + 1, :] / pixel_total
            shifted = (back[here, at] - shift).astype(BF16)
            centered = (fp[here, at].astype(F32) - mean).astype(BF16)
            out = jnp.dot(shifted, w_ref[k], preferred_element_type=F32) + jnp.dot(
                centered, s_ref[k], preferred_element_type=F32
            )
            o_ref[b, :, :, at] = out.astype(BF16).reshape(height, wide, LANES)[:, :width]

    pl.loop(0, images // 2)(final_part)
    for s in range(streams):
        finish(s, 3)
        if bits > 4:
            begin(s, 4)
    pl.loop(images // 2, images)(final_part)
    for t in range(4, bits):
        for s in range(streams):
            finish(s, t)
            if t + 1 < bits:
                begin(s, t + 1)

    mine = index * per // LANES
    mean = flat[pl.ds(base + blocks + mine, 1), :] / pixel_total
    whitened = jnp.dot(
        jnp.broadcast_to(mean, (8, LANES)), w_ref[mine].astype(F32),
        precision=highest, preferred_element_type=F32,
    )
    column[...] = across(whitened[:1])
    mean_part = column[pl.ds(pl.multiple_of(index * per % LANES, per), per), :]
    for s in range(streams):
        for q in range(part_width // LANES):
            at = s * (part_width // LANES) + q
            line = flat[base + 2 * blocks + at : base + 2 * blocks + at + 1, :]
            share_ref[:, at * LANES : (at + 1) * LANES] = (
                buffers[s][bits - 1][0, :, q * LANES : (q + 1) * LANES] - mean_part * line
            )


def pair_blocks(blocks):
    groups, size = blocks.shape[:2]
    pairs = blocks.reshape(groups // 2, 2, size, size)
    zero = jnp.zeros((groups // 2, size, size), blocks.dtype)
    top = jnp.concatenate([pairs[:, 0], zero], axis=2)
    bottom = jnp.concatenate([zero, pairs[:, 1]], axis=2)
    return jnp.concatenate([top, bottom], axis=1)


def general_local(shape, features, grads, kernel, vectors, values):
    images, height, width, channels = features.shape
    outputs = grads.shape[3]
    groups, group_size = values.shape
    devices = shape[0] * shape[1]
    bits = devices.bit_length() - 1
    orders = bit_orders(bits)
    per = channels // devices
    taps = 3 * outputs
    wide = round_up(width, 16)
    rows = images * height * wide
    kp = round_up(rows + 1, LANES)
    blocks = channels // LANES
    pixel_total = 1.0 * images * height * width * devices
    small_rows = channels // 2 + 2 * blocks + 3 * taps // LANES
    rp = round_up(-(-small_rows // devices), 8)

    streams = 6
    part_width = 3 * taps // streams
    lines = jnp.stack([lax.rsqrt(values), jnp.sqrt(values)]).reshape(2, blocks, LANES)
    vmem = pl.BlockSpec(memory_space=pltpu.VMEM)
    scratch = []
    for _ in range(streams):
        scratch += [pltpu.VMEM((devices >> (t + 1), per, part_width), F32) for t in range(bits)]
    scratch += [pltpu.VMEM((devices >> (t + 1), rp, LANES), F32) for t in range(bits)]
    sizes = (
        shape[0], shape[1], images, height, width, wide, channels, outputs, per, orders,
        streams, pixel_total,
    )
    input_grad, share = pl.pallas_call(
        functools.partial(general_kernel, sizes),
        out_shape=(
            jax.ShapeDtypeStruct(features.shape, BF16),
            jax.ShapeDtypeStruct((per, 3 * taps), F32),
        ),
        in_specs=[vmem, vmem, pl.BlockSpec(memory_space=pl.ANY), vmem, vmem],
        out_specs=(vmem, vmem),
        scratch_shapes=[
            pltpu.VMEM((kp, channels), BF16),
            pltpu.VMEM((channels, kp), BF16),
            pltpu.VMEM((kp, 3 * taps), BF16),
            pltpu.VMEM((height + 2, wide + 8, outputs), F32),
            pltpu.VMEM((3 * taps, channels), BF16),
            pltpu.VMEM((kp, channels), F32),
            pltpu.VMEM((blocks, LANES, LANES), BF16),
            pltpu.VMEM((blocks, LANES, LANES), BF16),
            pltpu.VMEM((devices * rp, LANES), F32),
            pltpu.VMEM((devices, rp, LANES), F32),
            pltpu.VMEM((devices, rp, LANES), F32),
            pltpu.VMEM((LANES, LANES), F32),
            pltpu.VMEM((streams, devices, per, part_width), F32),
            pltpu.SemaphoreType.DMA,
            pltpu.SemaphoreType.DMA((streams + 1, 2 * bits)),
            pltpu.SemaphoreType.DMA((streams + 1, 2 * bits)),
        ]
        + scratch,
        compiler_params=pltpu.CompilerParams(
            collective_id=0, has_side_effects=True, vmem_limit_bytes=VMEM_LIMIT
        ),
        name="step",
    )(features, grads, kernel.reshape(3 * taps, channels), pair_blocks(vectors), lines)
    return (input_grad, share.reshape(per, 3, 3, outputs))


PAIR, SHALLOW = 2, 2


def plan_kernel(
    sizes, f_ref, g_ref, k_hbm, v_ref, val_ref, o_ref, share_ref,
    fp, ft, cols, gpad, k_ref, back, w_ref, own_ref, s_ref, means,
    parts, swap, near1, near2, zsum, zin, zfar, early_in, early_far, early1, early2,
    total, mixed, mixed_in, stat, stat_in, stat_far, known, table,
    k_sem, send_sem, recv_sem, ready
):
    (images, height, width, wide, channels, outputs, group, depth, pixel_total) = sizes
    rows = images * height * wide
    kp = fp.shape[0]
    groups = channels // group
    blocks = channels // LANES
    tiles = 9
    taps = 3 * outputs
    quarter = group // 2
    plane = groups // depth
    image_rows = height * wide
    packed = quarter // 2

    batch = lax.axis_index("batch")
    row = lax.axis_index("rows")
    core = row % PAIR
    x = row // PAIR
    y = batch % SHALLOW
    z = batch // SHALLOW
    chip = (z * SHALLOW + y) * SHALLOW + x
    znear = z + 1 - 2 * (z % 2)
    zother = depth - 1 - z
    outer = (z == 0) | (z == depth - 1)
    inner = (z > 0) & (z < depth - 1)

    def place(x, y, z, core=core):
        return (z * SHALLOW + y, x * PAIR + core)

    partner = place(x, y, z, 1 - core)
    xside = place(1 - x, y, z)
    yside = place(x, 1 - y, z)

    def peer(k):
        px = 1 - x if k % 2 else x
        py = 1 - y if k // 2 % 2 else y
        low = 1 - z % 2 if k // 4 % 2 else z % 2
        high = 1 - z // 2 if k // 8 % 2 else z // 2
        pz = high * 2 + low
        return px, py, pz

    barrier = pltpu.get_barrier_semaphore()
    mesh_id = pl.DeviceIdType.MESH
    near = [xside, yside, place(x, y, znear)]
    count = len(near) + inner.astype(jnp.int32)

    def tell(sem, devices):
        for other in devices:
            pl.semaphore_signal(sem, inc=1, device_id=other, device_id_type=mesh_id)

        @pl.when(inner)
        def _():
            pl.semaphore_signal(
                sem, inc=1, device_id=place(x, y, zother), device_id_type=mesh_id
            )

    def spread(k):
        if k > 0:
            pl.semaphore_wait(ready.at[k - 1], count)
        tell(ready.at[k], near)

    def spread_done():
        pl.semaphore_wait(ready.at[3], count)

    tell(barrier, near + [partner])
    k_copy = pltpu.make_async_copy(k_hbm, k_ref, k_sem)
    k_copy.start()

    sems = {}

    def copy(key, src, dst, device, landing=None):
        at = sems.setdefault(key, len(sems))
        to = at if landing is None else sems.setdefault(landing, len(sems))
        return pltpu.make_async_remote_copy(
            src_ref=src, dst_ref=dst, send_sem=send_sem.at[at], recv_sem=recv_sem.at[to],
            device_id=device, device_id_type=pl.DeviceIdType.MESH,
        )

    flights = {}

    def send(key, src, dst, device):
        flights[key] = copy(key, src, dst, device)
        flights[key].start()

    def arrive(key):
        flights.pop(key).wait()

    fp[pl.ds(rows, kp - rows), :] = jnp.zeros((kp - rows, channels), BF16)
    cols[pl.ds(rows, kp - rows), :] = jnp.zeros((kp - rows, 3 * taps), BF16)
    gpad[...] = jnp.zeros(gpad.shape, F32)

    @pl.loop(0, images)
    def _(b):
        gpad[pl.ds(1, height), pl.ds(1, width), :] = g_ref[b].astype(F32)
        for h in range(height):
            at = pl.multiple_of((b * height + h) * wide, 16)
            fp[pl.ds(at, wide), :] = jnp.zeros((wide, channels), BF16)
            fp[pl.ds(at, width), :] = f_ref[b, h]
        at = pl.multiple_of(b * image_rows, 16)
        for c in range(3):
            shifted = gpad[:, 2 - c : 2 - c + wide, :].astype(BF16)
            for a in range(3):
                first = a * taps + c * outputs
                cols[pl.ds(at, image_rows), first : first + outputs] = shifted[
                    2 - a : 2 - a + height
                ].reshape(image_rows, outputs)

    @pl.loop(0, blocks)
    def _(k):
        at = pl.ds(pl.multiple_of(k * LANES, LANES), LANES)
        ft[at, :] = fp[:, at].T

    position = lax.broadcasted_iota(jnp.int32, (kp, 1), 0)
    valid = (position % wide < width) & (position < rows)
    lane = lax.broadcasted_iota(jnp.int32, (16, kp), 1)
    ft[pl.ds(channels, 16), :] = jnp.where(
        (lane % wide < width) & (lane < rows), 1.0, 0.0
    ).astype(BF16)
    stat[:, :, pl.ds(packed, 8), :] = jnp.zeros((PAIR, groups, 8, LANES), F32)

    first_plane = [0, 2, 4, 5, 6, 7, 8]
    first_depth = [1, 3]

    def slot(t, half, g):
        gz, gy, gx = g // 4, g // 2 % 2, g % 2
        first, second = (gx, gy) if half == 0 else (gy, gx)
        if t in first_depth:
            return gz * 4 + first * 2 + second
        return first * 8 + second * 4 + gz

    def tile(t):
        high = channels // 2
        for m in range(2):
            extra = 16 if m == 1 else 0
            part = jnp.dot(
                ft[m * high : (m + 1) * high + extra, :],
                cols[:, t * outputs : (t + 1) * outputs],
                preferred_element_type=F32,
            )
            for q in range(groups // 2):
                g = m * (groups // 2) + q
                for half in range(2):
                    lines = slice(q * group + half * quarter, q * group + (half + 1) * quarter)
                    for c in range(PAIR):
                        parts[t, c, half, slot(t, half, g)] = part[
                            lines, c * LANES : (c + 1) * LANES
                        ]
            if m == 1:
                for c in range(PAIR):
                    stat[c, t, packed + 1 : packed + 2, :] = part[
                        high : high + 1, c * LANES : (c + 1) * LANES
                    ]
        send(("swap", t), parts.at[t, 1 - core], swap.at[t], partner)

    def add(dst, src, dst_first, count, src_first=0):
        @pl.loop(0, count)
        def _(i):
            dst[dst_first + i] = dst[dst_first + i] + src[src_first + i]

    def mine(t, half):
        return parts.at[t, core, half]

    firsts = [(x, y), (y, x)]
    sides = [(xside, yside), (yside, xside)]

    def swapped(t):
        arrive(("swap", t))
        for half in range(2):
            add(mine(t, half), swap.at[t, half], 0, groups)

    def plane1(t):
        for half in range(2):
            send(
                ("p1", t, half),
                mine(t, half).at[pl.ds((1 - firsts[half][0]) * 8, 8)],
                near1.at[t, half], sides[half][0],
            )

    def plane2(t):
        for half in range(2):
            arrive(("p1", t, half))
            f, s = firsts[half]
            add(mine(t, half), near1.at[t, half], f * 8 + (1 - s) * 4, 4, (1 - s) * 4)
            send(
                ("p2", t, half),
                mine(t, half).at[pl.ds(f * 8 + (1 - s) * 4, 4)],
                near2.at[t, half], sides[half][1],
            )
        for half in range(2):
            f, s = firsts[half]
            add(mine(t, half), near1.at[t, half], f * 8 + s * 4, 4, s * 4)

    def depth1(t):
        for half in range(2):
            arrive(("p2", t, half))
            f, s = firsts[half]
            src = mine(t, half)
            for j in range(depth):
                zsum[t, j, pl.ds(half * quarter, quarter)] = (
                    src[f * 8 + s * 4 + j] + near2[t, half, j]
                )
        key = ("z1", t)

        @pl.when(outer)
        def _():
            copy(
                key, zsum.at[t, pl.ds((depth - 1 - z) // 3, 3)], zin.at[t], place(x, y, znear)
            ).start()

        @pl.when(inner)
        def _():
            copy(
                key, zsum.at[t, pl.ds(znear, 1)], zin.at[t, pl.ds(0, 1)], place(x, y, znear)
            ).start()

    def depth2(t):
        key = ("z1", t)

        @pl.when(outer)
        def _():
            near = place(x, y, znear)
            copy(key, zsum.at[t, pl.ds((depth - 1 - z) // 3, 3)], zin.at[t], near).wait_send()
            copy(key, zsum.at[t, pl.ds(0, 1)], zin.at[t, pl.ds(0, 1)], near).wait_recv()
            zsum[t, z] = zsum[t, z] + zin[t, 0]

        @pl.when(inner)
        def _():
            near = place(x, y, znear)
            copy(key, zsum.at[t, pl.ds(znear, 1)], zin.at[t, pl.ds(0, 1)], near).wait_send()
            copy(key, zsum.at[t, pl.ds(0, 3)], zin.at[t], near).wait_recv()
            for j in range(3):
                zsum[t, 2 - z + j] = zsum[t, 2 - z + j] + zin[t, j]
            copy(
                ("z2", t), zsum.at[t, pl.ds(zother, 1)], zfar.at[t], place(x, y, zother)
            ).start()
            zfin = 3 * (2 - z)
            copy(
                ("z3", t), zsum.at[t, pl.ds(zfin, 1)], zfar.at[t], place(x, y, zfin), ("z2", t)
            ).start()

    def depth3(t):
        @pl.when(inner)
        def _():
            copy(
                ("z2", t), zsum.at[t, pl.ds(zother, 1)], zfar.at[t], place(x, y, zother)
            ).wait_send()
            zfin = 3 * (2 - z)
            copy(
                ("z3", t), zsum.at[t, pl.ds(zfin, 1)], zfar.at[t], place(x, y, zfin), ("z2", t)
            ).wait_send()

        copy(
            ("z2", t), zsum.at[t, pl.ds(0, 1)], zfar.at[t], place(x, y, zother)
        ).wait_recv()
        total[t] = zsum[t, z] + zfar[t, 0]

    def early1_start(t, half):
        e = first_depth.index(t)
        key = ("e1", t, half)
        src = mine(t, half)

        @pl.when(outer)
        def _():
            copy(
                key, src.at[pl.ds((depth - 1 - z) // 3 * 4, 12)], early_in.at[e, half],
                place(x, y, znear),
            ).start()

        @pl.when(inner)
        def _():
            copy(
                key, src.at[pl.ds(znear * 4, 4)], early_in.at[e, half, pl.ds(0, 4)],
                place(x, y, znear),
            ).start()

    def early2_start(t, half):
        e = first_depth.index(t)
        key = ("e1", t, half)
        src = mine(t, half)
        buf = early_in.at[e, half]
        far = early_far.at[e, half]

        @pl.when(outer)
        def _():
            near = place(x, y, znear)
            copy(key, src.at[pl.ds((depth - 1 - z) // 3 * 4, 12)], buf, near).wait_send()
            copy(key, src.at[pl.ds(0, 4)], buf.at[pl.ds(0, 4)], near).wait_recv()
            add(src, buf, z * 4, 4)

        @pl.when(inner)
        def _():
            near = place(x, y, znear)
            copy(key, src.at[pl.ds(znear * 4, 4)], buf.at[pl.ds(0, 4)], near).wait_send()
            copy(key, src.at[pl.ds(0, 12)], buf, near).wait_recv()
            add(src, buf, (2 - z) * 4, 12)
            copy(
                ("e2", t, half), src.at[pl.ds(zother * 4, 4)], far, place(x, y, zother)
            ).start()
            zfin = 3 * (2 - z)
            copy(
                ("e3", t, half), src.at[pl.ds(zfin * 4, 4)], far, place(x, y, zfin),
                ("e2", t, half),
            ).start()

    def early3_start(t, half):
        e = first_depth.index(t)
        src = mine(t, half)
        far = early_far.at[e, half]

        @pl.when(inner)
        def _():
            copy(
                ("e2", t, half), src.at[pl.ds(zother * 4, 4)], far, place(x, y, zother)
            ).wait_send()
            zfin = 3 * (2 - z)
            copy(
                ("e3", t, half), src.at[pl.ds(zfin * 4, 4)], far, place(x, y, zfin),
                ("e2", t, half),
            ).wait_send()

        copy(("e2", t, half), src.at[pl.ds(0, 4)], far, place(x, y, zother)).wait_recv()
        add(src, far, z * 4, 4)
        send(
            ("e4", t, half),
            src.at[pl.ds(z * 4 + (1 - firsts[half][0]) * 2, 2)],
            early1.at[e, half], sides[half][0],
        )

    def early4_start(t, half):
        e = first_depth.index(t)
        arrive(("e4", t, half))
        f, s = firsts[half]
        src = mine(t, half)
        add(src, early1.at[e, half], z * 4 + f * 2, 2)
        send(
            ("e5", t, half),
            src.at[pl.ds(z * 4 + f * 2 + (1 - s), 1)],
            early2.at[e, half], sides[half][1],
        )

    def early5(t, half):
        e = first_depth.index(t)
        arrive(("e5", t, half))
        f, s = firsts[half]
        src = mine(t, half)
        total[t, pl.ds(half * quarter, quarter)] = (
            src[z * 4 + f * 2 + s] + early2[e, half, 0]
        )

    step = 2 * LANES
    half_rows = kp // 2
    low_lane = lax.broadcasted_iota(jnp.int32, (quarter, LANES), 1) < LANES // 2
    low_line = lax.broadcasted_iota(jnp.int32, (8, LANES), 1) < LANES // 2

    def turn(a):
        return pltpu.roll(a, LANES // 2, 1)

    def back_part(n, r):
        at = slice(n * step, (n + 1) * step)
        here = slice(r * half_rows, (r + 1) * half_rows)
        back[here, at] = jnp.dot(cols[here, :], k_ref[:, at], preferred_element_type=F32)

    def cov_part(n):
        at = slice(n * step, (n + 1) * step)
        grad = back[:, at]
        summed = jnp.broadcast_to(
            jnp.sum(jnp.where(valid, grad, 0.0), axis=0, keepdims=True), (8, step)
        )
        raw = jnp.dot(ft[at, :], grad.astype(BF16), preferred_element_type=F32)
        fsum = jnp.dot(ft[channels : channels + 16, :], fp[:, at], preferred_element_type=F32)[:8]
        for q in range(2):
            wide_at = slice(q * LANES, (q + 1) * LANES)
            block = raw[wide_at, wide_at]
            bs, fs = summed[:, wide_at], fsum[:, wide_at]
            g = (2 * n + q) * 2
            pieces = [block[i * quarter : (i + 1) * quarter] for i in range(4)]
            lower = jnp.where(low_lane, pieces[0], turn(pieces[1]))
            upper = jnp.where(low_lane, turn(pieces[2]), pieces[3])
            for c in range(PAIR):
                stat[c, g, :packed] = lower[c * packed : (c + 1) * packed]
                stat[c, g + 1, :packed] = upper[c * packed : (c + 1) * packed]
            stat[0, g, packed : packed + 1] = jnp.where(low_line, fs, turn(bs))[:1]
            stat[0, g + 1, packed : packed + 1] = jnp.where(low_line, turn(fs), bs)[:1]

    def stat1():
        send("s1", stat.at[1 - core], stat_in, partner)

    def stat2():
        arrive("s1")
        src = stat.at[core]
        add(src, stat_in, 0, groups)
        for k in range(1, groups):
            px, py, pz = peer(k)
            send(
                ("s2", k), src.at[(pz * SHALLOW + py) * SHALLOW + px], stat_far.at[k],
                place(px, py, pz),
            )

    def stat3():
        summed = stat[core, chip]
        for k in range(1, groups):
            arrive(("s2", k))
            summed = summed + stat_far[k]
        known[core] = summed
        send("s3", known.at[core], known.at[core], partner)

    def across(line):
        return jnp.broadcast_to(line, (LANES, LANES)).T[:group, :group]

    def hdot(a, b, dims):
        return lax.dot_general(
            a, b, (dims, ((), ())), precision=highest, preferred_element_type=F32
        )

    def stat4():
        arrive("s3")
        lines = jnp.concatenate([known[0, :packed], known[1, :packed]], axis=0)
        raw = jnp.concatenate([lines, turn(lines)], axis=0)[:, :group]
        both = jnp.broadcast_to(known[0, packed : packed + 1], (8, LANES))
        mean = both[:1] / pixel_total
        summed = turn(both)[:1, :group]
        cov = raw - across(mean) * summed
        v = v_ref[chip]
        vals = jnp.concatenate(
            [val_ref[pl.ds(chip, 1), :], jnp.ones((1, LANES - group), F32)], axis=1
        )
        scale = lax.rsqrt(vals)
        root = jnp.sqrt(vals)
        turned = hdot(v, cov, ((0,), (0,)))
        rotated = hdot(turned, v, ((1,), (0,)))
        symmetric = 0.5 * (rotated + rotated.T)
        factor = -(across(scale) * scale[:, :group]) / (across(root) + root[:, :group])
        inside = hdot(v, symmetric * factor, ((1,), (0,)))
        sigma = 2.0 / pixel_total * hdot(inside, v, ((1,), (1,)))
        own_ref[...] = hdot(v * scale[:, :group], v, ((1,), (1,))).astype(BF16)
        sigma = jnp.concatenate([sigma, jnp.zeros((group, LANES - group), F32)], axis=1)
        folded = jnp.where(low_lane, sigma[:quarter], turn(sigma[quarter:]))
        table[core, chip, :packed] = jnp.where(core == 0, folded[:packed], folded[packed:])
        table[core, chip, packed:] = known[core, packed:]
        table[core, chip, packed : packed + 1] = known[0, packed : packed + 1]
        src = table.at[core, chip]
        for k in range(1, groups):
            send(("s4", k), src, src, place(*peer(k)))

    def stat5():
        for k in range(1, groups):
            arrive(("s4", k))
        send("s5", table.at[core], table.at[core], partner)

    def stat6():
        arrive("s5")
        for k in range(blocks):
            folded = [
                jnp.concatenate([table[0, 2 * k + q, :packed], table[1, 2 * k + q, :packed]], axis=0)
                for q in range(2)
            ]
            s_ref[k] = jnp.concatenate(
                [
                    jnp.where(low_lane, folded[0], 0.0),
                    jnp.where(low_lane, turn(folded[0]), 0.0),
                    jnp.where(low_lane, 0.0, turn(folded[1])),
                    jnp.where(low_lane, 0.0, folded[1]),
                ],
                axis=0,
            ).astype(BF16)
            sums = [
                jnp.broadcast_to(table[0, 2 * k + q, packed : packed + 1], (8, LANES))
                for q in range(2)
            ]
            means[0, k] = jnp.where(low_line, sums[0], turn(sums[1])) / pixel_total
            means[1, k] = jnp.where(low_line, turn(sums[0]), sums[1]) / pixel_total

    def whiten_part(k):
        zero = jnp.zeros((group, LANES - group), F32)
        for q in range(2):
            g = 2 * k + q
            v = v_ref[g]
            scaled = v * lax.rsqrt(val_ref[g : g + 1, :])
            w = jnp.concatenate([hdot(scaled, v, ((1,), (1,))), zero], axis=1)
            if q == 1:
                w = turn(w)
            w_ref[k, q * group : (q + 1) * group, :] = w.astype(BF16)

    def final_part(b):
        here = pl.ds(pl.multiple_of(b * image_rows, 16), image_rows)
        for k in range(blocks):
            at = slice(k * LANES, (k + 1) * LANES)
            shifted = (back[here, at] - means[1, k, :1]).astype(BF16)
            centered = (fp[here, at].astype(F32) - means[0, k, :1]).astype(BF16)
            out = jnp.dot(shifted, w_ref[k], preferred_element_type=F32) + jnp.dot(
                centered, s_ref[k], preferred_element_type=F32
            )
            o_ref[b, :, :, at] = out.astype(BF16).reshape(height, wide, LANES)[:, :width]

    def whitened(t):
        both = known[0, packed : packed + 1] / pixel_total
        mean = jnp.broadcast_to(both, (LANES, LANES)).T[:group]
        block = total[t] - mean * table[core, t, packed + 1 : packed + 2]
        one = block.astype(BF16)
        left = block - one.astype(F32)
        two = left.astype(BF16)
        three = (left - two.astype(F32)).astype(BF16)
        weight = own_ref[...]
        mixed[t] = sum(
            lax.dot_general(weight, a, (((0,), (0,)), ((), ())), preferred_element_type=F32)
            for a in (one, two, three)
        )
        send(("m", t), mixed.at[t, pl.ds((1 - core) * quarter, quarter)], mixed_in.at[t], partner)
        here = pl.ds(pl.multiple_of(core * LANES, LANES), LANES)
        share_ref[t, :, here] = mixed[t, pl.ds(core * quarter, quarter)]

    def finished(t):
        arrive(("m", t))
        there = pl.ds(pl.multiple_of((1 - core) * LANES, LANES), LANES)
        share_ref[t, :, there] = mixed_in[t]

    p = first_plane
    e = first_depth
    pl.semaphore_wait(barrier, count + 1)
    spread(0)
    tile(p[0])
    spread(1)
    tile(e[0])
    spread(2)
    tile(p[1])
    spread(3)
    tile(e[1])
    spread_done()
    swapped(p[0])
    plane1(p[0])
    tile(p[2])
    swapped(e[0])
    swapped(p[1])
    plane1(p[1])
    early1_start(e[0], 0)
    early1_start(e[0], 1)
    tile(p[3])
    swapped(e[1])
    early1_start(e[1], 0)
    early1_start(e[1], 1)
    tile(p[4])
    swapped(p[2])
    plane1(p[2])
    tile(p[5])
    swapped(p[3])
    plane1(p[3])
    tile(p[6])
    plane2(p[0])
    swapped(p[4])
    k_copy.wait()
    back_part(0, 0)
    back_part(0, 1)
    early2_start(e[0], 0)
    cov_part(0)
    plane1(p[4])
    back_part(1, 0)
    back_part(1, 1)
    plane2(p[2])
    cov_part(1)
    back_part(2, 0)
    early2_start(e[0], 1)
    back_part(2, 1)
    plane2(p[3])
    cov_part(2)
    back_part(3, 0)
    depth1(p[0])
    back_part(3, 1)
    early2_start(e[1], 0)
    cov_part(3)
    stat1()
    whiten_part(7)
    plane2(p[4])
    early3_start(e[0], 1)
    whiten_part(5)
    whiten_part(0)
    whiten_part(1)
    whiten_part(6)
    stat2()
    depth1(p[2])
    early3_start(e[0], 0)
    plane2(p[1])
    whiten_part(3)
    whiten_part(4)
    early2_start(e[1], 1)
    depth1(p[3])
    swapped(p[5])
    plane1(p[5])
    swapped(p[6])
    whiten_part(2)
    early3_start(e[1], 0)
    depth1(p[4])
    depth2(p[0])
    early4_start(e[0], 1)
    plane1(p[6])
    early4_start(e[0], 0)
    depth1(p[1])
    depth2(p[2])
    early3_start(e[1], 1)
    stat3()
    plane2(p[5])
    early4_start(e[1], 0)
    stat4()
    depth2(p[3])
    depth3(p[0])
    depth3(p[2])
    depth2(p[4])
    early5(e[0], 0)
    early5(e[0], 1)
    plane2(p[6])
    early4_start(e[1], 1)
    depth2(p[1])
    depth1(p[5])
    early5(e[1], 0)
    early5(e[1], 1)
    depth1(p[6])
    depth3(p[3])
    depth2(p[5])
    stat5()
    depth3(p[4])
    depth3(p[1])
    stat6()
    whitened(p[2])
    depth2(p[6])
    whitened(p[4])
    final_part(1)
    final_part(3)
    depth3(p[5])
    whitened(p[5])
    final_part(5)
    whitened(p[1])
    whitened(e[1])
    whitened(e[0])
    finished(p[2])
    whitened(p[0])
    finished(p[5])
    final_part(0)
    whitened(p[3])
    finished(p[1])
    depth3(p[6])
    whitened(p[6])
    finished(e[0])
    finished(e[1])
    final_part(4)
    finished(p[0])
    final_part(2)
    finished(p[3])
    finished(p[4])
    finished(p[6])


def plan_local(shape, features, grads, kernel, vectors, values):
    images, height, width, channels = features.shape
    outputs = grads.shape[3]
    groups, group = values.shape
    devices = shape[0] * shape[1]
    depth = shape[0] // SHALLOW
    taps = 3 * outputs
    wide = round_up(width, 16)
    rows = images * height * wide
    kp = round_up(rows + 1, LANES)
    blocks = channels // LANES
    pixel_total = 1.0 * images * height * width * devices
    quarter = group // 2
    stat_rows = quarter // 2 + 8
    sizes = (images, height, width, wide, channels, outputs, group, depth, pixel_total)
    vmem = pl.BlockSpec(memory_space=pltpu.VMEM)
    sem_count = 192
    f32 = [
        (9, PAIR, 2, groups, quarter, LANES),
        (9, 2, groups, quarter, LANES),
        (9, 2, 8, quarter, LANES),
        (9, 2, 4, quarter, LANES),
        (9, depth, group, LANES),
        (9, 3, group, LANES),
        (9, 1, group, LANES),
        (2, 2, 12, quarter, LANES),
        (2, 2, 4, quarter, LANES),
        (2, 2, 2, quarter, LANES),
        (2, 2, 1, quarter, LANES),
        (9, group, LANES),
        (9, group, LANES),
        (9, quarter, LANES),
        (PAIR, groups, stat_rows, LANES),
        (groups, stat_rows, LANES),
        (groups, stat_rows, LANES),
        (PAIR, stat_rows, LANES),
        (PAIR, groups, stat_rows, LANES),
    ]
    input_grad, share = pl.pallas_call(
        functools.partial(plan_kernel, sizes),
        out_shape=(
            jax.ShapeDtypeStruct(features.shape, BF16),
            jax.ShapeDtypeStruct((9, channels // devices, outputs), F32),
        ),
        in_specs=[vmem, vmem, pl.BlockSpec(memory_space=pl.ANY), vmem, vmem],
        out_specs=(vmem, vmem),
        scratch_shapes=[
            pltpu.VMEM((kp, channels), BF16),
            pltpu.VMEM((channels + 16, kp), BF16),
            pltpu.VMEM((kp, 3 * taps), BF16),
            pltpu.VMEM((height + 2, wide + 8, outputs), F32),
            pltpu.VMEM((3 * taps, channels), BF16),
            pltpu.VMEM((kp, channels), F32),
            pltpu.VMEM((blocks, LANES, LANES), BF16),
            pltpu.VMEM((group, group), BF16),
            pltpu.VMEM((blocks, LANES, LANES), BF16),
            pltpu.VMEM((2, blocks, 8, LANES), F32),
        ]
        + [pltpu.VMEM(s, F32) for s in f32]
        + [
            pltpu.SemaphoreType.DMA,
            pltpu.SemaphoreType.DMA((sem_count,)),
            pltpu.SemaphoreType.DMA((sem_count,)),
            pltpu.SemaphoreType.REGULAR((4,)),
        ],
        compiler_params=pltpu.CompilerParams(
            collective_id=0, has_side_effects=True, vmem_limit_bytes=VMEM_LIMIT
        ),
        name="step",
    )(features, grads, kernel.reshape(3 * taps, channels), vectors, values)
    per = channels // devices
    return (input_grad, share.reshape(3, 3, per, outputs).transpose(2, 0, 1, 3))


def solution(mesh):
    shape = (mesh.shape["batch"], mesh.shape["rows"])
    split = P(("batch", "rows"), None, None, None)

    def local(features, grads, kernel, vectors, values):
        groups, group = values.shape
        fits = (
            shape == (SHALLOW * 4, PAIR * SHALLOW)
            and groups * PAIR == shape[0] * shape[1]
            and group * 2 == LANES
            and grads.shape[3] == PAIR * LANES
            and features.shape[0] % 3 == 0
        )
        body = plan_local if fits else general_local
        return body(shape, features, grads, kernel, vectors, values)

    return jax.shard_map(
        local,
        mesh=mesh,
        in_specs=(split, split, P(), P(), P()),
        out_specs=(split, split),
        check_vma=False,
    )
```

```python
import functools
import jax
import jax.numpy as jnp
from jax import lax
from jax.experimental import pallas as pl
from jax.experimental.pallas import tpu as pltpu
from jax.sharding import PartitionSpec as P

highest = lax.Precision.HIGHEST
F32, BF16 = jnp.float32, jnp.bfloat16
LANES = 128
VMEM_LIMIT = 63 * 1024 * 1024


def round_up(n, m):
    return (n + m - 1) // m * m


def bit_orders(bits):
    rest = list(range(1, bits))
    first = [0] + rest
    second = [0] + rest[1:2] + rest[:1] + rest[2:]
    third = [0] + rest[2:3] + rest[:2] + rest[3:]
    return [first, second, third]


def slot_of(index, order):
    slot = 0
    count = len(order)
    for step, bit in enumerate(order):
        slot = slot + (index // 2**bit) % 2 * 2 ** (count - 1 - step)
    return slot


def general_kernel(
    sizes, f_ref, g_ref, k_hbm, v_ref, sv_ref, o_ref, share_ref,
    fp, ft, cols, gpad, k_ref, back, w_ref, s_ref, flat, small, total, column, pieces,
    k_sem, send_sem, recv_sem, *scratch
):
    (nb, nr, images, height, width, wide, channels, outputs, per, orders, streams, pixel_total) = sizes
    rows = images * height * wide
    kp = fp.shape[0]
    blocks = channels // LANES
    taps = 3 * outputs
    part_width = 3 * taps // streams
    bits = len(orders[0])
    count = 2**bits
    rp = small.shape[1]
    half = LANES // 2
    base = channels // 2
    image_rows = height * wide
    batch = lax.axis_index("batch")
    row = lax.axis_index("rows")
    index = batch * nr + row

    def bit_of(bit):
        return (index // 2**bit) % 2

    def partner(bit):
        sign = 1 - 2 * bit_of(bit)
        if 2**bit < nr:
            return (batch, row + sign * 2**bit)
        return (batch + sign * (2**bit // nr), row)

    barrier = pltpu.get_barrier_semaphore()
    for bit in range(bits):
        pl.semaphore_signal(
            barrier, inc=1, device_id=partner(bit), device_id_type=pl.DeviceIdType.MESH
        )
    k_copy = pltpu.make_async_copy(k_hbm, k_ref, k_sem)
    k_copy.start()

    fp[pl.ds(rows, kp - rows), :] = jnp.zeros((kp - rows, channels), BF16)
    cols[pl.ds(rows, kp - rows), :] = jnp.zeros((kp - rows, 3 * taps), BF16)
    gpad[...] = jnp.zeros(gpad.shape, F32)

    @pl.loop(0, images)
    def _(b):
        gpad[pl.ds(1, height), pl.ds(1, width), :] = g_ref[b].astype(F32)
        for h in range(height):
            at = pl.multiple_of((b * height + h) * wide, 16)
            fp[pl.ds(at, wide), :] = jnp.zeros((wide, channels), BF16)
            fp[pl.ds(at, width), :] = f_ref[b, h]
        at = pl.multiple_of(b * image_rows, 16)
        for c in range(3):
            shifted = gpad[:, 2 - c : 2 - c + wide, :].astype(BF16)
            for a in range(3):
                first = a * taps + c * outputs
                cols[pl.ds(at, image_rows), first : first + outputs] = shifted[
                    2 - a : 2 - a + height
                ].reshape(image_rows, outputs)

    @pl.loop(0, blocks)
    def _(k):
        at = pl.ds(pl.multiple_of(k * LANES, LANES), LANES)
        ft[at, :] = fp[:, at].T
        v = v_ref[k]
        w_ref[k] = lax.dot_general(
            v * sv_ref[0, pl.ds(k, 1), :], v, (((1,), (1,)), ((), ())),
            precision=highest, preferred_element_type=F32,
        ).astype(BF16)

    position = lax.broadcasted_iota(jnp.int32, (kp, 1), 0)
    valid = (position % wide < width) & (position < rows)
    lane = lax.broadcasted_iota(jnp.int32, (8, kp), 1)
    ones = jnp.where((lane % wide < width) & (lane < rows), 1.0, 0.0).astype(BF16)
    low_lane = lax.broadcasted_iota(jnp.int32, (half, LANES), 1) < half
    flat[pl.ds(base, flat.shape[0] - base), :] = jnp.zeros((flat.shape[0] - base, LANES), F32)

    def copy(src, dst, s, t, bit):
        c = pltpu.make_async_remote_copy(
            src_ref=src,
            dst_ref=dst,
            send_sem=send_sem.at[s, t],
            recv_sem=recv_sem.at[s, t],
            device_id=partner(bit),
            device_id_type=pl.DeviceIdType.MESH,
        )
        c.start()
        return c

    sources = [pieces.at[s] for s in range(streams)] + [small]
    buffers = [[scratch[s * bits + t] for t in range(bits)] for s in range(streams + 1)]
    all_orders = [orders[s % 3] for s in range(streams)] + [orders[0]]
    flights = {}

    def begin(s, t):
        bit = all_orders[s][t]
        size = count >> (t + 1)
        src = sources[s] if t == 0 else buffers[s][t - 1]
        flights[s] = copy(
            src.at[pl.ds((1 - bit_of(bit)) * size, size)], buffers[s][t], s, t, bit
        )

    def finish(s, t):
        size = count >> (t + 1)
        src = sources[s] if t == 0 else buffers[s][t - 1]
        dst = buffers[s][t]
        flights[s].wait()
        first = bit_of(all_orders[s][t]) * size

        @pl.loop(0, size)
        def _(i):
            dst[i] = dst[i] + src[first + i]

    slot = slot_of(index, all_orders[streams])

    def spread(u):
        region = pl.ds(slot // 2**u * 2**u, 2**u)
        flights[streams] = copy(
            total.at[region], total.at[region], streams, bits + u,
            all_orders[streams][bits - 1 - u],
        )

    def advance(t):
        if t < bits:
            finish(streams, t)
            if t + 1 < bits:
                begin(streams, t + 1)
            else:
                total[slot] = buffers[streams][t][0]
                spread(0)
        else:
            flights[streams].wait()
            if t + 1 < 2 * bits:
                spread(t + 1 - bits)

    def piece(s):
        high = 4 * LANES

        @pl.loop(0, channels // high)
        def _(m):
            at = pl.ds(pl.multiple_of(m * high, high), high)
            part = jnp.dot(
                ft[at, :],
                cols[:, s * part_width : (s + 1) * part_width],
                preferred_element_type=F32,
            )
            for q in range(4):
                weight = w_ref[4 * m + q]
                block = part[q * LANES : (q + 1) * LANES]
                one = block.astype(BF16)
                left = block - one.astype(F32)
                two = left.astype(BF16)
                three = (left - two.astype(F32)).astype(BF16)
                result = sum(
                    lax.dot_general(
                        weight, x, (((0,), (0,)), ((), ())), preferred_element_type=F32
                    )
                    for x in (one, two, three)
                )
                for j in range(LANES // per):
                    chunk = (4 * m + q) * (LANES // per) + j
                    pieces[s, slot_of(chunk, all_orders[s])] = result[j * per : (j + 1) * per]

    step = 2 * LANES

    def back_part(n):
        at = pl.ds(pl.multiple_of(n * step, step), step)
        grad = jnp.dot(cols[...], k_ref[:, at], preferred_element_type=F32)
        back[:, at] = grad
        summed = jnp.sum(jnp.where(valid, grad, 0.0), axis=0, keepdims=True)
        low = grad.astype(BF16)
        raw = jnp.dot(ft[at, :], low, preferred_element_type=F32)
        fsum = jnp.dot(ones, fp[:, at], preferred_element_type=F32)
        for q in range(2):
            block = raw[q * LANES : (q + 1) * LANES, q * LANES : (q + 1) * LANES]
            where = pl.multiple_of((2 * n + q) * half, half)
            flat[pl.ds(where, half), :] = jnp.where(low_lane, block[:half], block[half:])
            flat[pl.ds(base + 2 * n + q, 1), :] = summed[:, q * LANES : (q + 1) * LANES]
            flat[pl.ds(base + blocks + 2 * n + q, 1), :] = fsum[:1, q * LANES : (q + 1) * LANES]

    def pack_sums():
        colsum = jnp.dot(ones, cols[...], preferred_element_type=F32)
        for q in range(3 * taps // LANES):
            flat[pl.ds(base + 2 * blocks + q, 1), :] = colsum[:1, q * LANES : (q + 1) * LANES]

        @pl.loop(0, count)
        def _(i):
            small[i] = flat[pl.ds(pl.multiple_of(i * rp, 8), rp), :]

    pl.semaphore_wait(barrier, bits)
    for s in range(streams):
        piece(s)
        begin(s, 0)
        if s > 0:
            finish(s - 1, 0)
            begin(s - 1, 1)
    finish(streams - 1, 0)
    begin(streams - 1, 1)
    k_copy.wait()
    turns = channels // step
    pl.loop(0, turns // 2)(back_part)
    for s in range(streams // 2):
        finish(s, 1)
        begin(s, 2)
    pl.loop(turns // 2, turns)(back_part)
    pack_sums()
    begin(streams, 0)
    done = 0
    for t in (1, 2):
        for s in range(streams):
            if t == 2 or s >= streams // 2:
                finish(s, t)
                begin(s, t + 1)
                if done < 2 * bits:
                    advance(done)
                    done += 1
    while done < 2 * bits:
        advance(done)
        done += 1

    @pl.loop(0, count)
    def _(i):
        flat[pl.ds(pl.multiple_of(i * rp, 8), rp), :] = total[i]

    def across(line):
        return jnp.broadcast_to(line, (LANES, LANES)).T

    side = lax.broadcasted_iota(jnp.int32, (LANES, LANES), 0) < half
    other = lax.broadcasted_iota(jnp.int32, (LANES, LANES), 1) < half
    inside = side == other

    @pl.loop(0, blocks)
    def _(k):
        packed = flat[pl.ds(pl.multiple_of(k * half, half), half), :]
        mean = flat[pl.ds(base + blocks + k, 1), :] / pixel_total
        summed = flat[pl.ds(base + k, 1), :]
        raw = jnp.concatenate([packed, packed], axis=0)
        cov = jnp.where(inside, raw - across(mean) * summed, 0.0)
        v = v_ref[k]
        scale = sv_ref[0, pl.ds(k, 1), :]
        root = sv_ref[1, pl.ds(k, 1), :]
        turned = lax.dot_general(
            v, cov, (((0,), (0,)), ((), ())), precision=highest, preferred_element_type=F32
        )
        rotated = jnp.dot(turned, v, precision=highest, preferred_element_type=F32)
        symmetric = 0.5 * (rotated + rotated.T)
        factor = -(across(scale) * scale) / (across(root) + root)
        inner = jnp.where(inside, symmetric * factor, 0.0)
        outer = jnp.dot(v, inner, precision=highest, preferred_element_type=F32)
        sigma = lax.dot_general(
            outer, v, (((1,), (1,)), ((), ())), precision=highest, preferred_element_type=F32
        )
        s_ref[k] = (2.0 / pixel_total * sigma).astype(BF16)

    def final_part(b):
        here = pl.ds(pl.multiple_of(b * image_rows, 16), image_rows)
        for k in range(blocks):
            at = slice(k * LANES, (k + 1) * LANES)
            mean = flat[base + blocks + k : base + blocks + k + 1, :] / pixel_total
            shift = flat[base + k : base + k + 1, :] / pixel_total
            shifted = (back[here, at] - shift).astype(BF16)
            centered = (fp[here, at].astype(F32) - mean).astype(BF16)
            out = jnp.dot(shifted, w_ref[k], preferred_element_type=F32) + jnp.dot(
                centered, s_ref[k], preferred_element_type=F32
            )
            o_ref[b, :, :, at] = out.astype(BF16).reshape(height, wide, LANES)[:, :width]

    pl.loop(0, images // 2)(final_part)
    for s in range(streams):
        finish(s, 3)
        if bits > 4:
            begin(s, 4)
    pl.loop(images // 2, images)(final_part)
    for t in range(4, bits):
        for s in range(streams):
            finish(s, t)
            if t + 1 < bits:
                begin(s, t + 1)

    mine = index * per // LANES
    mean = flat[pl.ds(base + blocks + mine, 1), :] / pixel_total
    whitened = jnp.dot(
        jnp.broadcast_to(mean, (8, LANES)), w_ref[mine].astype(F32),
        precision=highest, preferred_element_type=F32,
    )
    column[...] = across(whitened[:1])
    mean_part = column[pl.ds(pl.multiple_of(index * per % LANES, per), per), :]
    for s in range(streams):
        for q in range(part_width // LANES):
            at = s * (part_width // LANES) + q
            line = flat[base + 2 * blocks + at : base + 2 * blocks + at + 1, :]
            share_ref[:, at * LANES : (at + 1) * LANES] = (
                buffers[s][bits - 1][0, :, q * LANES : (q + 1) * LANES] - mean_part * line
            )


def pair_blocks(blocks):
    groups, size = blocks.shape[:2]
    pairs = blocks.reshape(groups // 2, 2, size, size)
    zero = jnp.zeros((groups // 2, size, size), blocks.dtype)
    top = jnp.concatenate([pairs[:, 0], zero], axis=2)
    bottom = jnp.concatenate([zero, pairs[:, 1]], axis=2)
    return jnp.concatenate([top, bottom], axis=1)


def general_local(shape, features, grads, kernel, vectors, values):
    images, height, width, channels = features.shape
    outputs = grads.shape[3]
    groups, group_size = values.shape
    devices = shape[0] * shape[1]
    bits = devices.bit_length() - 1
    orders = bit_orders(bits)
    per = channels // devices
    taps = 3 * outputs
    wide = round_up(width, 16)
    rows = images * height * wide
    kp = round_up(rows + 1, LANES)
    blocks = channels // LANES
    pixel_total = 1.0 * images * height * width * devices
    small_rows = channels // 2 + 2 * blocks + 3 * taps // LANES
    rp = round_up(-(-small_rows // devices), 8)

    streams = 6
    part_width = 3 * taps // streams
    lines = jnp.stack([lax.rsqrt(values), jnp.sqrt(values)]).reshape(2, blocks, LANES)
    vmem = pl.BlockSpec(memory_space=pltpu.VMEM)
    scratch = []
    for _ in range(streams):
        scratch += [pltpu.VMEM((devices >> (t + 1), per, part_width), F32) for t in range(bits)]
    scratch += [pltpu.VMEM((devices >> (t + 1), rp, LANES), F32) for t in range(bits)]
    sizes = (
        shape[0], shape[1], images, height, width, wide, channels, outputs, per, orders,
        streams, pixel_total,
    )
    input_grad, share = pl.pallas_call(
        functools.partial(general_kernel, sizes),
        out_shape=(
            jax.ShapeDtypeStruct(features.shape, BF16),
            jax.ShapeDtypeStruct((per, 3 * taps), F32),
        ),
        in_specs=[vmem, vmem, pl.BlockSpec(memory_space=pl.ANY), vmem, vmem],
        out_specs=(vmem, vmem),
        scratch_shapes=[
            pltpu.VMEM((kp, channels), BF16),
            pltpu.VMEM((channels, kp), BF16),
            pltpu.VMEM((kp, 3 * taps), BF16),
            pltpu.VMEM((height + 2, wide + 8, outputs), F32),
            pltpu.VMEM((3 * taps, channels), BF16),
            pltpu.VMEM((kp, channels), F32),
            pltpu.VMEM((blocks, LANES, LANES), BF16),
            pltpu.VMEM((blocks, LANES, LANES), BF16),
            pltpu.VMEM((devices * rp, LANES), F32),
            pltpu.VMEM((devices, rp, LANES), F32),
            pltpu.VMEM((devices, rp, LANES), F32),
            pltpu.VMEM((LANES, LANES), F32),
            pltpu.VMEM((streams, devices, per, part_width), F32),
            pltpu.SemaphoreType.DMA,
            pltpu.SemaphoreType.DMA((streams + 1, 2 * bits)),
            pltpu.SemaphoreType.DMA((streams + 1, 2 * bits)),
        ]
        + scratch,
        compiler_params=pltpu.CompilerParams(
            collective_id=0, has_side_effects=True, vmem_limit_bytes=VMEM_LIMIT
        ),
        name="step",
    )(features, grads, kernel.reshape(3 * taps, channels), pair_blocks(vectors), lines)
    return (input_grad, share.reshape(per, 3, 3, outputs))


PAIR, SHALLOW = 2, 2


def plan_kernel(
    sizes, f_hbm, g_hbm, k_hbm, v_hbm, val_hbm, o_hbm, share_hbm,
    f_ref, g_ref, v_ref, val_ref, o_ref, share_ref,
    fp, ft, cols, gpad, k_ref, back, w_ref, own_ref, s_ref, means,
    parts, swap, near1, near2, zsum, zin, zfar, early_in, early_far, early1, early2,
    total, mixed, mixed_in, stat, stat_in, stat_far, known, table,
    k_sem, f_sem, o_sem, send_sem, recv_sem, ready
):
    (images, height, width, wide, channels, outputs, group, depth, pixel_total) = sizes
    rows = images * height * wide
    kp = fp.shape[0]
    groups = channels // group
    blocks = channels // LANES
    tiles = 9
    taps = 3 * outputs
    quarter = group // 2
    plane = groups // depth
    image_rows = height * wide
    packed = quarter // 2

    batch = lax.axis_index("batch")
    row = lax.axis_index("rows")
    core = row % PAIR
    x = row // PAIR
    y = batch % SHALLOW
    z = batch // SHALLOW
    chip = (z * SHALLOW + y) * SHALLOW + x
    znear = z + 1 - 2 * (z % 2)
    zother = depth - 1 - z
    outer = (z == 0) | (z == depth - 1)
    inner = (z > 0) & (z < depth - 1)

    def place(x, y, z, core=core):
        return (z * SHALLOW + y, x * PAIR + core)

    partner = place(x, y, z, 1 - core)
    xside = place(1 - x, y, z)
    yside = place(x, 1 - y, z)

    def peer(k):
        px = 1 - x if k % 2 else x
        py = 1 - y if k // 2 % 2 else y
        low = 1 - z % 2 if k // 4 % 2 else z % 2
        high = 1 - z // 2 if k // 8 % 2 else z // 2
        pz = high * 2 + low
        return px, py, pz

    barrier = pltpu.get_barrier_semaphore()
    mesh_id = pl.DeviceIdType.MESH
    near = [xside, yside, place(x, y, znear)]
    count = len(near) + inner.astype(jnp.int32)

    def tell(sem, devices):
        for other in devices:
            pl.semaphore_signal(sem, inc=1, device_id=other, device_id_type=mesh_id)

        @pl.when(inner)
        def _():
            pl.semaphore_signal(
                sem, inc=1, device_id=place(x, y, zother), device_id_type=mesh_id
            )

    def spread(k):
        if k > 0:
            pl.semaphore_wait(ready.at[k - 1], count)
        tell(ready.at[k], near)

    def spread_done():
        pl.semaphore_wait(ready.at[3], count)

    tell(barrier, near + [partner])
    k_copy = pltpu.make_async_copy(k_hbm, k_ref, k_sem)
    g_copy = pltpu.make_async_copy(g_hbm, g_ref, f_sem.at[0])
    f_copy = pltpu.make_async_copy(f_hbm, f_ref, f_sem.at[1])
    v_copy = pltpu.make_async_copy(v_hbm, v_ref, f_sem.at[2])
    val_copy = pltpu.make_async_copy(val_hbm, val_ref, f_sem.at[3])
    for load in (g_copy, f_copy, v_copy, val_copy):
        load.start()

    sems = {}

    def copy(key, src, dst, device, landing=None):
        at = sems.setdefault(key, len(sems))
        to = at if landing is None else sems.setdefault(landing, len(sems))
        return pltpu.make_async_remote_copy(
            src_ref=src, dst_ref=dst, send_sem=send_sem.at[at], recv_sem=recv_sem.at[to],
            device_id=device, device_id_type=pl.DeviceIdType.MESH,
        )

    flights = {}

    def send(key, src, dst, device):
        flights[key] = copy(key, src, dst, device)
        flights[key].start()

    def arrive(key):
        flights.pop(key).wait()

    fp[pl.ds(rows, kp - rows), :] = jnp.zeros((kp - rows, channels), BF16)
    cols[pl.ds(rows, kp - rows), :] = jnp.zeros((kp - rows, 3 * taps), BF16)
    gpad[...] = jnp.zeros(gpad.shape, F32)

    g_copy.wait()

    @pl.loop(0, images)
    def _(b):
        gpad[pl.ds(1, height), pl.ds(1, width), :] = g_ref[b].astype(F32)
        at = pl.multiple_of(b * image_rows, 16)
        for c in range(3):
            shifted = gpad[:, 2 - c : 2 - c + wide, :].astype(BF16)
            for a in range(3):
                first = a * taps + c * outputs
                cols[pl.ds(at, image_rows), first : first + outputs] = shifted[
                    2 - a : 2 - a + height
                ].reshape(image_rows, outputs)

    f_copy.wait()
    k_copy.start()

    @pl.loop(0, images)
    def _(b):
        for h in range(height):
            at = pl.multiple_of((b * height + h) * wide, 16)
            fp[pl.ds(at, wide), :] = jnp.zeros((wide, channels), BF16)
            fp[pl.ds(at, width), :] = f_ref[b, h]

    @pl.loop(0, blocks)
    def _(k):
        at = pl.ds(pl.multiple_of(k * LANES, LANES), LANES)
        ft[at, :] = fp[:, at].T

    position = lax.broadcasted_iota(jnp.int32, (kp, 1), 0)
    valid = (position % wide < width) & (position < rows)
    lane = lax.broadcasted_iota(jnp.int32, (16, kp), 1)
    ft[pl.ds(channels, 16), :] = jnp.where(
        (lane % wide < width) & (lane < rows), 1.0, 0.0
    ).astype(BF16)
    stat[:, :, pl.ds(packed, 8), :] = jnp.zeros((PAIR, groups, 8, LANES), F32)

    first_plane = [0, 2, 4, 5, 6, 7, 8]
    first_depth = [1, 3]

    def slot(t, half, g):
        gz, gy, gx = g // 4, g // 2 % 2, g % 2
        first, second = (gx, gy) if half == 0 else (gy, gx)
        if t in first_depth:
            return gz * 4 + first * 2 + second
        return first * 8 + second * 4 + gz

    def tile(t):
        high = channels // 2
        for m in range(2):
            extra = 16 if m == 1 else 0
            part = jnp.dot(
                ft[m * high : (m + 1) * high + extra, :],
                cols[:, t * outputs : (t + 1) * outputs],
                preferred_element_type=F32,
            )
            for q in range(groups // 2):
                g = m * (groups // 2) + q
                for half in range(2):
                    lines = slice(q * group + half * quarter, q * group + (half + 1) * quarter)
                    for c in range(PAIR):
                        parts[t, c, half, slot(t, half, g)] = part[
                            lines, c * LANES : (c + 1) * LANES
                        ]
            if m == 1:
                for c in range(PAIR):
                    stat[c, t, packed + 1 : packed + 2, :] = part[
                        high : high + 1, c * LANES : (c + 1) * LANES
                    ]
        send(("swap", t), parts.at[t, 1 - core], swap.at[t], partner)

    def add(dst, src, dst_first, count, src_first=0):
        for i in range(count):
            dst[dst_first + i] = dst[dst_first + i] + src[src_first + i]

    def mine(t, half):
        return parts.at[t, core, half]

    firsts = [(x, y), (y, x)]
    sides = [(xside, yside), (yside, xside)]

    def swapped(t):
        arrive(("swap", t))
        for half in range(2):
            dst, src = mine(t, half), swap.at[t, half]

            @pl.loop(0, groups, step=8)
            def _(i):
                for j in range(8):
                    dst[i + j] = dst[i + j] + src[i + j]

    def plane1(t):
        for half in range(2):
            send(
                ("p1", t, half),
                mine(t, half).at[pl.ds((1 - firsts[half][0]) * 8, 8)],
                near1.at[t, half], sides[half][0],
            )

    def plane2(t):
        for half in range(2):
            arrive(("p1", t, half))
            f, s = firsts[half]
            add(mine(t, half), near1.at[t, half], f * 8 + (1 - s) * 4, 4, (1 - s) * 4)
            send(
                ("p2", t, half),
                mine(t, half).at[pl.ds(f * 8 + (1 - s) * 4, 4)],
                near2.at[t, half], sides[half][1],
            )
        for half in range(2):
            f, s = firsts[half]
            add(mine(t, half), near1.at[t, half], f * 8 + s * 4, 4, s * 4)

    def depth1(t):
        for half in range(2):
            arrive(("p2", t, half))
            f, s = firsts[half]
            src = mine(t, half)
            for j in range(depth):
                zsum[t, j, pl.ds(half * quarter, quarter)] = (
                    src[f * 8 + s * 4 + j] + near2[t, half, j]
                )
        key = ("z1", t)

        @pl.when(outer)
        def _():
            copy(
                key, zsum.at[t, pl.ds((depth - 1 - z) // 3, 3)], zin.at[t], place(x, y, znear)
            ).start()

        @pl.when(inner)
        def _():
            copy(
                key, zsum.at[t, pl.ds(znear, 1)], zin.at[t, pl.ds(0, 1)], place(x, y, znear)
            ).start()

    def depth2(t):
        key = ("z1", t)

        @pl.when(outer)
        def _():
            near = place(x, y, znear)
            copy(key, zsum.at[t, pl.ds((depth - 1 - z) // 3, 3)], zin.at[t], near).wait_send()
            copy(key, zsum.at[t, pl.ds(0, 1)], zin.at[t, pl.ds(0, 1)], near).wait_recv()
            zsum[t, z] = zsum[t, z] + zin[t, 0]

        @pl.when(inner)
        def _():
            near = place(x, y, znear)
            copy(key, zsum.at[t, pl.ds(znear, 1)], zin.at[t, pl.ds(0, 1)], near).wait_send()
            copy(key, zsum.at[t, pl.ds(0, 3)], zin.at[t], near).wait_recv()
            for j in range(3):
                zsum[t, 2 - z + j] = zsum[t, 2 - z + j] + zin[t, j]
            copy(
                ("z2", t), zsum.at[t, pl.ds(zother, 1)], zfar.at[t], place(x, y, zother)
            ).start()
            zfin = 3 * (2 - z)
            copy(
                ("z3", t), zsum.at[t, pl.ds(zfin, 1)], zfar.at[t], place(x, y, zfin), ("z2", t)
            ).start()

    def depth3(t):
        @pl.when(inner)
        def _():
            copy(
                ("z2", t), zsum.at[t, pl.ds(zother, 1)], zfar.at[t], place(x, y, zother)
            ).wait_send()
            zfin = 3 * (2 - z)
            copy(
                ("z3", t), zsum.at[t, pl.ds(zfin, 1)], zfar.at[t], place(x, y, zfin), ("z2", t)
            ).wait_send()

        copy(
            ("z2", t), zsum.at[t, pl.ds(0, 1)], zfar.at[t], place(x, y, zother)
        ).wait_recv()
        total[t] = zsum[t, z] + zfar[t, 0]

    def early1_start(t, half):
        e = first_depth.index(t)
        key = ("e1", t, half)
        src = mine(t, half)

        @pl.when(outer)
        def _():
            copy(
                key, src.at[pl.ds((depth - 1 - z) // 3 * 4, 12)], early_in.at[e, half],
                place(x, y, znear),
            ).start()

        @pl.when(inner)
        def _():
            copy(
                key, src.at[pl.ds(znear * 4, 4)], early_in.at[e, half, pl.ds(0, 4)],
                place(x, y, znear),
            ).start()

    def early2_start(t, half):
        e = first_depth.index(t)
        key = ("e1", t, half)
        src = mine(t, half)
        buf = early_in.at[e, half]
        far = early_far.at[e, half]

        @pl.when(outer)
        def _():
            near = place(x, y, znear)
            copy(key, src.at[pl.ds((depth - 1 - z) // 3 * 4, 12)], buf, near).wait_send()
            copy(key, src.at[pl.ds(0, 4)], buf.at[pl.ds(0, 4)], near).wait_recv()
            add(src, buf, z * 4, 4)

        @pl.when(inner)
        def _():
            near = place(x, y, znear)
            copy(key, src.at[pl.ds(znear * 4, 4)], buf.at[pl.ds(0, 4)], near).wait_send()
            copy(key, src.at[pl.ds(0, 12)], buf, near).wait_recv()
            add(src, buf, (2 - z) * 4, 12)
            copy(
                ("e2", t, half), src.at[pl.ds(zother * 4, 4)], far, place(x, y, zother)
            ).start()
            zfin = 3 * (2 - z)
            copy(
                ("e3", t, half), src.at[pl.ds(zfin * 4, 4)], far, place(x, y, zfin),
                ("e2", t, half),
            ).start()

    def early3_start(t, half):
        e = first_depth.index(t)
        src = mine(t, half)
        far = early_far.at[e, half]

        @pl.when(inner)
        def _():
            copy(
                ("e2", t, half), src.at[pl.ds(zother * 4, 4)], far, place(x, y, zother)
            ).wait_send()
            zfin = 3 * (2 - z)
            copy(
                ("e3", t, half), src.at[pl.ds(zfin * 4, 4)], far, place(x, y, zfin),
                ("e2", t, half),
            ).wait_send()

        copy(("e2", t, half), src.at[pl.ds(0, 4)], far, place(x, y, zother)).wait_recv()
        add(src, far, z * 4, 4)
        send(
            ("e4", t, half),
            src.at[pl.ds(z * 4 + (1 - firsts[half][0]) * 2, 2)],
            early1.at[e, half], sides[half][0],
        )

    def early4_start(t, half):
        e = first_depth.index(t)
        arrive(("e4", t, half))
        f, s = firsts[half]
        src = mine(t, half)
        add(src, early1.at[e, half], z * 4 + f * 2, 2)
        send(
            ("e5", t, half),
            src.at[pl.ds(z * 4 + f * 2 + (1 - s), 1)],
            early2.at[e, half], sides[half][1],
        )

    def early5(t, half):
        e = first_depth.index(t)
        arrive(("e5", t, half))
        f, s = firsts[half]
        src = mine(t, half)
        total[t, pl.ds(half * quarter, quarter)] = (
            src[z * 4 + f * 2 + s] + early2[e, half, 0]
        )

    step = 2 * LANES
    half_rows = kp // 2
    low_lane = lax.broadcasted_iota(jnp.int32, (quarter, LANES), 1) < LANES // 2
    low_line = lax.broadcasted_iota(jnp.int32, (8, LANES), 1) < LANES // 2

    def turn(a):
        return pltpu.roll(a, LANES // 2, 1)

    def back_part(n, r):
        at = slice(n * step, (n + 1) * step)
        here = slice(r * half_rows, (r + 1) * half_rows)
        back[here, at] = jnp.dot(cols[here, :], k_ref[:, at], preferred_element_type=F32)

    def cov_part(n):
        at = slice(n * step, (n + 1) * step)
        grad = back[:, at]
        summed = jnp.broadcast_to(
            jnp.sum(jnp.where(valid, grad, 0.0), axis=0, keepdims=True), (8, step)
        )
        raw = jnp.dot(ft[at, :], grad.astype(BF16), preferred_element_type=F32)
        fsum = jnp.dot(ft[channels : channels + 16, :], fp[:, at], preferred_element_type=F32)[:8]
        for q in range(2):
            wide_at = slice(q * LANES, (q + 1) * LANES)
            block = raw[wide_at, wide_at]
            bs, fs = summed[:, wide_at], fsum[:, wide_at]
            g = (2 * n + q) * 2
            pieces = [block[i * quarter : (i + 1) * quarter] for i in range(4)]
            lower = jnp.where(low_lane, pieces[0], turn(pieces[1]))
            upper = jnp.where(low_lane, turn(pieces[2]), pieces[3])
            for c in range(PAIR):
                stat[c, g, :packed] = lower[c * packed : (c + 1) * packed]
                stat[c, g + 1, :packed] = upper[c * packed : (c + 1) * packed]
            stat[0, g, packed : packed + 1] = jnp.where(low_line, fs, turn(bs))[:1]
            stat[0, g + 1, packed : packed + 1] = jnp.where(low_line, turn(fs), bs)[:1]

    def stat1():
        send("s1", stat.at[1 - core], stat_in, partner)

    def stat2():
        arrive("s1")
        src = stat.at[core]
        add(src, stat_in, 0, groups)
        for k in range(1, groups):
            px, py, pz = peer(k)
            send(
                ("s2", k), src.at[(pz * SHALLOW + py) * SHALLOW + px], stat_far.at[k],
                place(px, py, pz),
            )

    def stat3():
        summed = stat[core, chip]
        for k in range(1, groups):
            arrive(("s2", k))
            summed = summed + stat_far[k]
        known[core] = summed
        send("s3", known.at[core], known.at[core], partner)

    def across(line):
        return jnp.broadcast_to(line, (LANES, LANES)).T[:group, :group]

    def hdot(a, b, dims):
        return lax.dot_general(
            a, b, (dims, ((), ())), precision=highest, preferred_element_type=F32
        )

    def stat4():
        arrive("s3")
        lines = jnp.concatenate([known[0, :packed], known[1, :packed]], axis=0)
        raw = jnp.concatenate([lines, turn(lines)], axis=0)[:, :group]
        both = jnp.broadcast_to(known[0, packed : packed + 1], (8, LANES))
        mean = both[:1] / pixel_total
        summed = turn(both)[:1, :group]
        cov = raw - across(mean) * summed
        v = v_ref[chip]
        vals = jnp.concatenate(
            [val_ref[pl.ds(chip, 1), :], jnp.ones((1, LANES - group), F32)], axis=1
        )
        scale = lax.rsqrt(vals)
        root = jnp.sqrt(vals)
        turned = hdot(v, cov, ((0,), (0,)))
        rotated = hdot(turned, v, ((1,), (0,)))
        symmetric = 0.5 * (rotated + rotated.T)
        factor = -(across(scale) * scale[:, :group]) / (across(root) + root[:, :group])
        inside = hdot(v, symmetric * factor, ((1,), (0,)))
        sigma = 2.0 / pixel_total * hdot(inside, v, ((1,), (1,)))
        own_ref[...] = hdot(v * scale[:, :group], v, ((1,), (1,))).astype(BF16)
        sigma = jnp.concatenate([sigma, jnp.zeros((group, LANES - group), F32)], axis=1)
        folded = jnp.where(low_lane, sigma[:quarter], turn(sigma[quarter:]))
        table[core, chip, :packed] = jnp.where(core == 0, folded[:packed], folded[packed:])
        table[core, chip, packed:] = known[core, packed:]
        table[core, chip, packed : packed + 1] = known[0, packed : packed + 1]
        src = table.at[core, chip]
        for k in range(1, groups):
            send(("s4", k), src, src, place(*peer(k)))

    def stat5():
        for k in range(1, groups):
            arrive(("s4", k))
        send("s5", table.at[core], table.at[core], partner)

    def stat6():
        arrive("s5")
        for k in range(blocks):
            folded = [
                jnp.concatenate([table[0, 2 * k + q, :packed], table[1, 2 * k + q, :packed]], axis=0)
                for q in range(2)
            ]
            s_ref[k] = jnp.concatenate(
                [
                    jnp.where(low_lane, folded[0], 0.0),
                    jnp.where(low_lane, turn(folded[0]), 0.0),
                    jnp.where(low_lane, 0.0, turn(folded[1])),
                    jnp.where(low_lane, 0.0, folded[1]),
                ],
                axis=0,
            ).astype(BF16)
            sums = [
                jnp.broadcast_to(table[0, 2 * k + q, packed : packed + 1], (8, LANES))
                for q in range(2)
            ]
            means[0, k] = jnp.where(low_line, sums[0], turn(sums[1])) / pixel_total
            means[1, k] = jnp.where(low_line, turn(sums[0]), sums[1]) / pixel_total

    def whiten_part(k):
        zero = jnp.zeros((group, LANES - group), F32)
        for q in range(2):
            g = 2 * k + q
            v = v_ref[g]
            scaled = v * lax.rsqrt(val_ref[g : g + 1, :])
            w = jnp.concatenate([hdot(scaled, v, ((1,), (1,))), zero], axis=1)
            if q == 1:
                w = turn(w)
            w_ref[k, q * group : (q + 1) * group, :] = w.astype(BF16)

    def final_part(b):
        here = pl.ds(pl.multiple_of(b * image_rows, 16), image_rows)
        for k in range(blocks):
            at = slice(k * LANES, (k + 1) * LANES)
            shifted = (back[here, at] - means[1, k, :1]).astype(BF16)
            centered = (fp[here, at].astype(F32) - means[0, k, :1]).astype(BF16)
            out = jnp.dot(shifted, w_ref[k], preferred_element_type=F32) + jnp.dot(
                centered, s_ref[k], preferred_element_type=F32
            )
            o_ref[b, :, :, at] = out.astype(BF16).reshape(height, wide, LANES)[:, :width]

    puts = []

    def put(b):
        puts.append(pltpu.make_async_copy(o_ref.at[b], o_hbm.at[b], o_sem.at[b]))
        puts[-1].start()

    def whitened(t):
        both = known[0, packed : packed + 1] / pixel_total
        mean = jnp.broadcast_to(both, (LANES, LANES)).T[:group]
        block = total[t] - mean * table[core, t, packed + 1 : packed + 2]
        one = block.astype(BF16)
        left = block - one.astype(F32)
        two = left.astype(BF16)
        three = (left - two.astype(F32)).astype(BF16)
        weight = own_ref[...]
        mixed[t] = sum(
            lax.dot_general(weight, a, (((0,), (0,)), ((), ())), preferred_element_type=F32)
            for a in (one, two, three)
        )
        send(("m", t), mixed.at[t, pl.ds((1 - core) * quarter, quarter)], mixed_in.at[t], partner)
        here = pl.ds(pl.multiple_of(core * LANES, LANES), LANES)
        share_ref[t, :, here] = mixed[t, pl.ds(core * quarter, quarter)]

    def finished(t):
        arrive(("m", t))
        there = pl.ds(pl.multiple_of((1 - core) * LANES, LANES), LANES)
        share_ref[t, :, there] = mixed_in[t]
        puts.append(
            pltpu.make_async_copy(share_ref.at[t], share_hbm.at[t], o_sem.at[images + t])
        )
        puts[-1].start()

    p = first_plane
    e = first_depth
    pl.semaphore_wait(barrier, count + 1)
    spread(0)
    tile(p[0])
    spread(1)
    tile(e[0])
    spread(2)
    tile(p[1])
    spread(3)
    tile(e[1])
    spread_done()
    swapped(p[0])
    plane1(p[0])
    tile(p[2])
    swapped(e[0])
    swapped(p[1])
    plane1(p[1])
    early1_start(e[0], 0)
    early1_start(e[0], 1)
    tile(p[3])
    swapped(e[1])
    early1_start(e[1], 0)
    early1_start(e[1], 1)
    tile(p[4])
    swapped(p[2])
    plane1(p[2])
    tile(p[5])
    swapped(p[3])
    plane1(p[3])
    tile(p[6])
    plane2(p[0])
    swapped(p[4])
    k_copy.wait()
    v_copy.wait()
    val_copy.wait()
    back_part(0, 0)
    back_part(0, 1)
    early2_start(e[0], 0)
    cov_part(0)
    plane1(p[4])
    back_part(1, 0)
    back_part(1, 1)
    plane2(p[2])
    cov_part(1)
    back_part(2, 0)
    early2_start(e[0], 1)
    back_part(2, 1)
    plane2(p[3])
    cov_part(2)
    back_part(3, 0)
    depth1(p[0])
    back_part(3, 1)
    early2_start(e[1], 0)
    cov_part(3)
    stat1()
    whiten_part(7)
    plane2(p[4])
    early3_start(e[0], 1)
    whiten_part(5)
    whiten_part(0)
    whiten_part(1)
    whiten_part(6)
    stat2()
    depth1(p[2])
    early3_start(e[0], 0)
    plane2(p[1])
    whiten_part(3)
    whiten_part(4)
    early2_start(e[1], 1)
    depth1(p[3])
    swapped(p[5])
    plane1(p[5])
    swapped(p[6])
    whiten_part(2)
    early3_start(e[1], 0)
    depth1(p[4])
    depth2(p[0])
    early4_start(e[0], 1)
    plane1(p[6])
    early4_start(e[0], 0)
    depth1(p[1])
    depth2(p[2])
    early3_start(e[1], 1)
    stat3()
    plane2(p[5])
    early4_start(e[1], 0)
    stat4()
    depth2(p[3])
    depth3(p[0])
    depth3(p[2])
    depth2(p[4])
    early5(e[0], 0)
    early5(e[0], 1)
    plane2(p[6])
    early4_start(e[1], 1)
    depth2(p[1])
    depth1(p[5])
    early5(e[1], 0)
    early5(e[1], 1)
    depth1(p[6])
    depth3(p[3])
    depth2(p[5])
    stat5()
    depth3(p[4])
    depth3(p[1])
    stat6()
    whitened(p[2])
    depth2(p[6])
    whitened(p[4])
    final_part(1)
    put(1)
    final_part(3)
    put(3)
    depth3(p[5])
    whitened(p[5])
    final_part(5)
    put(5)
    whitened(p[1])
    whitened(e[1])
    whitened(e[0])
    finished(p[2])
    whitened(p[0])
    finished(p[5])
    final_part(0)
    put(0)
    whitened(p[3])
    finished(p[1])
    depth3(p[6])
    whitened(p[6])
    finished(e[0])
    finished(e[1])
    final_part(4)
    put(4)
    finished(p[0])
    final_part(2)
    put(2)
    finished(p[3])
    finished(p[4])
    finished(p[6])
    for move in puts:
        move.wait()


def place_kernel(held, share, placed, given, page, sheet, sems):
    count = held.shape[0]
    pairs = [(share, sheet, given)]
    pairs += [(held.at[b], page.at[b], placed.at[b]) for b in range(count)]
    loads = [
        pltpu.make_async_copy(src, mid, sems.at[0, i]) for i, (src, mid, _) in enumerate(pairs)
    ]
    stores = [
        pltpu.make_async_copy(mid, dst, sems.at[1, i]) for i, (_, mid, dst) in enumerate(pairs)
    ]
    for load in loads:
        load.start()
    for load, store in zip(loads, stores):
        load.wait()
        store.start()
    for store in stores:
        store.wait()


def plan_local(shape, features, grads, kernel, vectors, values):
    images, height, width, channels = features.shape
    outputs = grads.shape[3]
    groups, group = values.shape
    devices = shape[0] * shape[1]
    depth = shape[0] // SHALLOW
    taps = 3 * outputs
    wide = round_up(width, 16)
    rows = images * height * wide
    kp = round_up(rows + 1, LANES)
    blocks = channels // LANES
    pixel_total = 1.0 * images * height * width * devices
    quarter = group // 2
    stat_rows = quarter // 2 + 8
    sizes = (images, height, width, wide, channels, outputs, group, depth, pixel_total)
    anywhere = pl.BlockSpec(memory_space=pl.ANY)
    sem_count = 192
    f32 = [
        (9, PAIR, 2, groups, quarter, LANES),
        (9, 2, groups, quarter, LANES),
        (9, 2, 8, quarter, LANES),
        (9, 2, 4, quarter, LANES),
        (9, depth, group, LANES),
        (9, 3, group, LANES),
        (9, 1, group, LANES),
        (2, 2, 12, quarter, LANES),
        (2, 2, 4, quarter, LANES),
        (2, 2, 2, quarter, LANES),
        (2, 2, 1, quarter, LANES),
        (9, group, LANES),
        (9, group, LANES),
        (9, quarter, LANES),
        (PAIR, groups, stat_rows, LANES),
        (groups, stat_rows, LANES),
        (groups, stat_rows, LANES),
        (PAIR, stat_rows, LANES),
        (PAIR, groups, stat_rows, LANES),
    ]
    held, share = pl.pallas_call(
        functools.partial(plan_kernel, sizes),
        out_shape=(
            jax.ShapeDtypeStruct(features.shape, BF16),
            jax.ShapeDtypeStruct((9, channels // devices, outputs), F32),
        ),
        in_specs=[anywhere] * 5,
        out_specs=(anywhere, anywhere),
        scratch_shapes=[
            pltpu.VMEM(features.shape, BF16),
            pltpu.VMEM(grads.shape, BF16),
            pltpu.VMEM(vectors.shape, F32),
            pltpu.VMEM(values.shape, F32),
            pltpu.VMEM(features.shape, BF16),
            pltpu.VMEM((9, channels // devices, outputs), F32),
            pltpu.VMEM((kp, channels), BF16),
            pltpu.VMEM((channels + 16, kp), BF16),
            pltpu.VMEM((kp, 3 * taps), BF16),
            pltpu.VMEM((height + 2, wide + 8, outputs), F32),
            pltpu.VMEM((3 * taps, channels), BF16),
            pltpu.VMEM((kp, channels), F32),
            pltpu.VMEM((blocks, LANES, LANES), BF16),
            pltpu.VMEM((group, group), BF16),
            pltpu.VMEM((blocks, LANES, LANES), BF16),
            pltpu.VMEM((2, blocks, 8, LANES), F32),
        ]
        + [pltpu.VMEM(s, F32) for s in f32]
        + [
            pltpu.SemaphoreType.DMA,
            pltpu.SemaphoreType.DMA((4,)),
            pltpu.SemaphoreType.DMA((images + 9,)),
            pltpu.SemaphoreType.DMA((sem_count,)),
            pltpu.SemaphoreType.DMA((sem_count,)),
            pltpu.SemaphoreType.REGULAR((4,)),
        ],
        compiler_params=pltpu.CompilerParams(
            collective_id=0, has_side_effects=True, vmem_limit_bytes=VMEM_LIMIT
        ),
        name="step",
    )(features, grads, kernel.reshape(3 * taps, channels), vectors, values)
    per = channels // devices
    input_grad, share = pl.pallas_call(
        place_kernel,
        out_shape=(
            jax.ShapeDtypeStruct(features.shape, BF16),
            jax.ShapeDtypeStruct((9, per, outputs), F32),
        ),
        in_specs=[anywhere, anywhere],
        out_specs=(anywhere, anywhere),
        scratch_shapes=[
            pltpu.VMEM(features.shape, BF16),
            pltpu.VMEM((9, per, outputs), F32),
            pltpu.SemaphoreType.DMA((2, images + 1)),
        ],
        compiler_params=pltpu.CompilerParams(vmem_limit_bytes=VMEM_LIMIT),
        name="place",
    )(held, share)
    return (input_grad, share.reshape(3, 3, per, outputs).transpose(2, 0, 1, 3))


def solution(mesh):
    shape = (mesh.shape["batch"], mesh.shape["rows"])
    split = P(("batch", "rows"), None, None, None)

    def local(features, grads, kernel, vectors, values):
        groups, group = values.shape
        fits = (
            shape == (SHALLOW * 4, PAIR * SHALLOW)
            and groups * PAIR == shape[0] * shape[1]
            and group * 2 == LANES
            and grads.shape[3] == PAIR * LANES
            and features.shape[0] % 3 == 0
        )
        body = plan_local if fits else general_local
        return body(shape, features, grads, kernel, vectors, values)

    return jax.shard_map(
        local,
        mesh=mesh,
        in_specs=(split, split, P(), P(), P()),
        out_specs=(split, split),
        check_vma=False,
    )
```

```python
import functools
import jax
import jax.numpy as jnp
from jax import lax
from jax.experimental import pallas as pl
from jax.experimental.pallas import tpu as pltpu
from jax.sharding import PartitionSpec as P

highest = lax.Precision.HIGHEST
F32, BF16 = jnp.float32, jnp.bfloat16
LANES = 128
VMEM_LIMIT = 63 * 1024 * 1024


def round_up(n, m):
    return (n + m - 1) // m * m


def bit_orders(bits):
    rest = list(range(1, bits))
    first = [0] + rest
    second = [0] + rest[1:2] + rest[:1] + rest[2:]
    third = [0] + rest[2:3] + rest[:2] + rest[3:]
    return [first, second, third]


def slot_of(index, order):
    slot = 0
    count = len(order)
    for step, bit in enumerate(order):
        slot = slot + (index // 2**bit) % 2 * 2 ** (count - 1 - step)
    return slot


def general_kernel(
    sizes, f_ref, g_ref, k_hbm, v_ref, sv_ref, o_ref, share_ref,
    fp, ft, cols, gpad, k_ref, back, w_ref, s_ref, flat, small, total, column, pieces,
    k_sem, send_sem, recv_sem, *scratch
):
    (nb, nr, images, height, width, wide, channels, outputs, per, orders, streams, pixel_total) = sizes
    rows = images * height * wide
    kp = fp.shape[0]
    blocks = channels // LANES
    taps = 3 * outputs
    part_width = 3 * taps // streams
    bits = len(orders[0])
    count = 2**bits
    rp = small.shape[1]
    half = LANES // 2
    base = channels // 2
    image_rows = height * wide
    batch = lax.axis_index("batch")
    row = lax.axis_index("rows")
    index = batch * nr + row

    def bit_of(bit):
        return (index // 2**bit) % 2

    def partner(bit):
        sign = 1 - 2 * bit_of(bit)
        if 2**bit < nr:
            return (batch, row + sign * 2**bit)
        return (batch + sign * (2**bit // nr), row)

    barrier = pltpu.get_barrier_semaphore()
    for bit in range(bits):
        pl.semaphore_signal(
            barrier, inc=1, device_id=partner(bit), device_id_type=pl.DeviceIdType.MESH
        )
    k_copy = pltpu.make_async_copy(k_hbm, k_ref, k_sem)
    k_copy.start()

    fp[pl.ds(rows, kp - rows), :] = jnp.zeros((kp - rows, channels), BF16)
    cols[pl.ds(rows, kp - rows), :] = jnp.zeros((kp - rows, 3 * taps), BF16)
    gpad[...] = jnp.zeros(gpad.shape, F32)

    @pl.loop(0, images)
    def _(b):
        gpad[pl.ds(1, height), pl.ds(1, width), :] = g_ref[b].astype(F32)
        for h in range(height):
            at = pl.multiple_of((b * height + h) * wide, 16)
            fp[pl.ds(at, wide), :] = jnp.zeros((wide, channels), BF16)
            fp[pl.ds(at, width), :] = f_ref[b, h]
        at = pl.multiple_of(b * image_rows, 16)
        for c in range(3):
            shifted = gpad[:, 2 - c : 2 - c + wide, :].astype(BF16)
            for a in range(3):
                first = a * taps + c * outputs
                cols[pl.ds(at, image_rows), first : first + outputs] = shifted[
                    2 - a : 2 - a + height
                ].reshape(image_rows, outputs)

    @pl.loop(0, blocks)
    def _(k):
        at = pl.ds(pl.multiple_of(k * LANES, LANES), LANES)
        ft[at, :] = fp[:, at].T
        v = v_ref[k]
        w_ref[k] = lax.dot_general(
            v * sv_ref[0, pl.ds(k, 1), :], v, (((1,), (1,)), ((), ())),
            precision=highest, preferred_element_type=F32,
        ).astype(BF16)

    position = lax.broadcasted_iota(jnp.int32, (kp, 1), 0)
    valid = (position % wide < width) & (position < rows)
    lane = lax.broadcasted_iota(jnp.int32, (8, kp), 1)
    ones = jnp.where((lane % wide < width) & (lane < rows), 1.0, 0.0).astype(BF16)
    low_lane = lax.broadcasted_iota(jnp.int32, (half, LANES), 1) < half
    flat[pl.ds(base, flat.shape[0] - base), :] = jnp.zeros((flat.shape[0] - base, LANES), F32)

    def copy(src, dst, s, t, bit):
        c = pltpu.make_async_remote_copy(
            src_ref=src,
            dst_ref=dst,
            send_sem=send_sem.at[s, t],
            recv_sem=recv_sem.at[s, t],
            device_id=partner(bit),
            device_id_type=pl.DeviceIdType.MESH,
        )
        c.start()
        return c

    sources = [pieces.at[s] for s in range(streams)] + [small]
    buffers = [[scratch[s * bits + t] for t in range(bits)] for s in range(streams + 1)]
    all_orders = [orders[s % 3] for s in range(streams)] + [orders[0]]
    flights = {}

    def begin(s, t):
        bit = all_orders[s][t]
        size = count >> (t + 1)
        src = sources[s] if t == 0 else buffers[s][t - 1]
        flights[s] = copy(
            src.at[pl.ds((1 - bit_of(bit)) * size, size)], buffers[s][t], s, t, bit
        )

    def finish(s, t):
        size = count >> (t + 1)
        src = sources[s] if t == 0 else buffers[s][t - 1]
        dst = buffers[s][t]
        flights[s].wait()
        first = bit_of(all_orders[s][t]) * size

        @pl.loop(0, size)
        def _(i):
            dst[i] = dst[i] + src[first + i]

    slot = slot_of(index, all_orders[streams])

    def spread(u):
        region = pl.ds(slot // 2**u * 2**u, 2**u)
        flights[streams] = copy(
            total.at[region], total.at[region], streams, bits + u,
            all_orders[streams][bits - 1 - u],
        )

    def advance(t):
        if t < bits:
            finish(streams, t)
            if t + 1 < bits:
                begin(streams, t + 1)
            else:
                total[slot] = buffers[streams][t][0]
                spread(0)
        else:
            flights[streams].wait()
            if t + 1 < 2 * bits:
                spread(t + 1 - bits)

    def piece(s):
        high = 4 * LANES

        @pl.loop(0, channels // high)
        def _(m):
            at = pl.ds(pl.multiple_of(m * high, high), high)
            part = jnp.dot(
                ft[at, :],
                cols[:, s * part_width : (s + 1) * part_width],
                preferred_element_type=F32,
            )
            for q in range(4):
                weight = w_ref[4 * m + q]
                block = part[q * LANES : (q + 1) * LANES]
                one = block.astype(BF16)
                left = block - one.astype(F32)
                two = left.astype(BF16)
                three = (left - two.astype(F32)).astype(BF16)
                result = sum(
                    lax.dot_general(
                        weight, x, (((0,), (0,)), ((), ())), preferred_element_type=F32
                    )
                    for x in (one, two, three)
                )
                for j in range(LANES // per):
                    chunk = (4 * m + q) * (LANES // per) + j
                    pieces[s, slot_of(chunk, all_orders[s])] = result[j * per : (j + 1) * per]

    step = 2 * LANES

    def back_part(n):
        at = pl.ds(pl.multiple_of(n * step, step), step)
        grad = jnp.dot(cols[...], k_ref[:, at], preferred_element_type=F32)
        back[:, at] = grad
        summed = jnp.sum(jnp.where(valid, grad, 0.0), axis=0, keepdims=True)
        low = grad.astype(BF16)
        raw = jnp.dot(ft[at, :], low, preferred_element_type=F32)
        fsum = jnp.dot(ones, fp[:, at], preferred_element_type=F32)
        for q in range(2):
            block = raw[q * LANES : (q + 1) * LANES, q * LANES : (q + 1) * LANES]
            where = pl.multiple_of((2 * n + q) * half, half)
            flat[pl.ds(where, half), :] = jnp.where(low_lane, block[:half], block[half:])
            flat[pl.ds(base + 2 * n + q, 1), :] = summed[:, q * LANES : (q + 1) * LANES]
            flat[pl.ds(base + blocks + 2 * n + q, 1), :] = fsum[:1, q * LANES : (q + 1) * LANES]

    def pack_sums():
        colsum = jnp.dot(ones, cols[...], preferred_element_type=F32)
        for q in range(3 * taps // LANES):
            flat[pl.ds(base + 2 * blocks + q, 1), :] = colsum[:1, q * LANES : (q + 1) * LANES]

        @pl.loop(0, count)
        def _(i):
            small[i] = flat[pl.ds(pl.multiple_of(i * rp, 8), rp), :]

    pl.semaphore_wait(barrier, bits)
    for s in range(streams):
        piece(s)
        begin(s, 0)
        if s > 0:
            finish(s - 1, 0)
            begin(s - 1, 1)
    finish(streams - 1, 0)
    begin(streams - 1, 1)
    k_copy.wait()
    turns = channels // step
    pl.loop(0, turns // 2)(back_part)
    for s in range(streams // 2):
        finish(s, 1)
        begin(s, 2)
    pl.loop(turns // 2, turns)(back_part)
    pack_sums()
    begin(streams, 0)
    done = 0
    for t in (1, 2):
        for s in range(streams):
            if t == 2 or s >= streams // 2:
                finish(s, t)
                begin(s, t + 1)
                if done < 2 * bits:
                    advance(done)
                    done += 1
    while done < 2 * bits:
        advance(done)
        done += 1

    @pl.loop(0, count)
    def _(i):
        flat[pl.ds(pl.multiple_of(i * rp, 8), rp), :] = total[i]

    def across(line):
        return jnp.broadcast_to(line, (LANES, LANES)).T

    side = lax.broadcasted_iota(jnp.int32, (LANES, LANES), 0) < half
    other = lax.broadcasted_iota(jnp.int32, (LANES, LANES), 1) < half
    inside = side == other

    @pl.loop(0, blocks)
    def _(k):
        packed = flat[pl.ds(pl.multiple_of(k * half, half), half), :]
        mean = flat[pl.ds(base + blocks + k, 1), :] / pixel_total
        summed = flat[pl.ds(base + k, 1), :]
        raw = jnp.concatenate([packed, packed], axis=0)
        cov = jnp.where(inside, raw - across(mean) * summed, 0.0)
        v = v_ref[k]
        scale = sv_ref[0, pl.ds(k, 1), :]
        root = sv_ref[1, pl.ds(k, 1), :]
        turned = lax.dot_general(
            v, cov, (((0,), (0,)), ((), ())), precision=highest, preferred_element_type=F32
        )
        rotated = jnp.dot(turned, v, precision=highest, preferred_element_type=F32)
        symmetric = 0.5 * (rotated + rotated.T)
        factor = -(across(scale) * scale) / (across(root) + root)
        inner = jnp.where(inside, symmetric * factor, 0.0)
        outer = jnp.dot(v, inner, precision=highest, preferred_element_type=F32)
        sigma = lax.dot_general(
            outer, v, (((1,), (1,)), ((), ())), precision=highest, preferred_element_type=F32
        )
        s_ref[k] = (2.0 / pixel_total * sigma).astype(BF16)

    def final_part(b):
        here = pl.ds(pl.multiple_of(b * image_rows, 16), image_rows)
        for k in range(blocks):
            at = slice(k * LANES, (k + 1) * LANES)
            mean = flat[base + blocks + k : base + blocks + k + 1, :] / pixel_total
            shift = flat[base + k : base + k + 1, :] / pixel_total
            shifted = (back[here, at] - shift).astype(BF16)
            centered = (fp[here, at].astype(F32) - mean).astype(BF16)
            out = jnp.dot(shifted, w_ref[k], preferred_element_type=F32) + jnp.dot(
                centered, s_ref[k], preferred_element_type=F32
            )
            o_ref[b, :, :, at] = out.astype(BF16).reshape(height, wide, LANES)[:, :width]

    pl.loop(0, images // 2)(final_part)
    for s in range(streams):
        finish(s, 3)
        if bits > 4:
            begin(s, 4)
    pl.loop(images // 2, images)(final_part)
    for t in range(4, bits):
        for s in range(streams):
            finish(s, t)
            if t + 1 < bits:
                begin(s, t + 1)

    mine = index * per // LANES
    mean = flat[pl.ds(base + blocks + mine, 1), :] / pixel_total
    whitened = jnp.dot(
        jnp.broadcast_to(mean, (8, LANES)), w_ref[mine].astype(F32),
        precision=highest, preferred_element_type=F32,
    )
    column[...] = across(whitened[:1])
    mean_part = column[pl.ds(pl.multiple_of(index * per % LANES, per), per), :]
    for s in range(streams):
        for q in range(part_width // LANES):
            at = s * (part_width // LANES) + q
            line = flat[base + 2 * blocks + at : base + 2 * blocks + at + 1, :]
            share_ref[:, at * LANES : (at + 1) * LANES] = (
                buffers[s][bits - 1][0, :, q * LANES : (q + 1) * LANES] - mean_part * line
            )


def pair_blocks(blocks):
    groups, size = blocks.shape[:2]
    pairs = blocks.reshape(groups // 2, 2, size, size)
    zero = jnp.zeros((groups // 2, size, size), blocks.dtype)
    top = jnp.concatenate([pairs[:, 0], zero], axis=2)
    bottom = jnp.concatenate([zero, pairs[:, 1]], axis=2)
    return jnp.concatenate([top, bottom], axis=1)


def general_local(shape, features, grads, kernel, vectors, values):
    images, height, width, channels = features.shape
    outputs = grads.shape[3]
    groups, group_size = values.shape
    devices = shape[0] * shape[1]
    bits = devices.bit_length() - 1
    orders = bit_orders(bits)
    per = channels // devices
    taps = 3 * outputs
    wide = round_up(width, 16)
    rows = images * height * wide
    kp = round_up(rows + 1, LANES)
    blocks = channels // LANES
    pixel_total = 1.0 * images * height * width * devices
    small_rows = channels // 2 + 2 * blocks + 3 * taps // LANES
    rp = round_up(-(-small_rows // devices), 8)

    streams = 6
    part_width = 3 * taps // streams
    lines = jnp.stack([lax.rsqrt(values), jnp.sqrt(values)]).reshape(2, blocks, LANES)
    vmem = pl.BlockSpec(memory_space=pltpu.VMEM)
    scratch = []
    for _ in range(streams):
        scratch += [pltpu.VMEM((devices >> (t + 1), per, part_width), F32) for t in range(bits)]
    scratch += [pltpu.VMEM((devices >> (t + 1), rp, LANES), F32) for t in range(bits)]
    sizes = (
        shape[0], shape[1], images, height, width, wide, channels, outputs, per, orders,
        streams, pixel_total,
    )
    input_grad, share = pl.pallas_call(
        functools.partial(general_kernel, sizes),
        out_shape=(
            jax.ShapeDtypeStruct(features.shape, BF16),
            jax.ShapeDtypeStruct((per, 3 * taps), F32),
        ),
        in_specs=[vmem, vmem, pl.BlockSpec(memory_space=pl.ANY), vmem, vmem],
        out_specs=(vmem, vmem),
        scratch_shapes=[
            pltpu.VMEM((kp, channels), BF16),
            pltpu.VMEM((channels, kp), BF16),
            pltpu.VMEM((kp, 3 * taps), BF16),
            pltpu.VMEM((height + 2, wide + 8, outputs), F32),
            pltpu.VMEM((3 * taps, channels), BF16),
            pltpu.VMEM((kp, channels), F32),
            pltpu.VMEM((blocks, LANES, LANES), BF16),
            pltpu.VMEM((blocks, LANES, LANES), BF16),
            pltpu.VMEM((devices * rp, LANES), F32),
            pltpu.VMEM((devices, rp, LANES), F32),
            pltpu.VMEM((devices, rp, LANES), F32),
            pltpu.VMEM((LANES, LANES), F32),
            pltpu.VMEM((streams, devices, per, part_width), F32),
            pltpu.SemaphoreType.DMA,
            pltpu.SemaphoreType.DMA((streams + 1, 2 * bits)),
            pltpu.SemaphoreType.DMA((streams + 1, 2 * bits)),
        ]
        + scratch,
        compiler_params=pltpu.CompilerParams(
            collective_id=0, has_side_effects=True, vmem_limit_bytes=VMEM_LIMIT
        ),
        name="step",
    )(features, grads, kernel.reshape(3 * taps, channels), pair_blocks(vectors), lines)
    return (input_grad, share.reshape(per, 3, 3, outputs))


PAIR, SHALLOW = 2, 2


def plan_kernel(
    sizes, f_hbm, g_hbm, k_hbm, v_hbm, val_hbm, o_hbm, share_hbm,
    f_ref, g_ref, v_ref, val_ref, o_ref, share_ref,
    fp, ft, cols, gpad, k_ref, back, w_ref, own_ref, s_ref, means,
    parts, swap, near1, near2, zsum, zin, zfar, early_in, early_far, early1, early2,
    total, mixed, mixed_in, stat, stat_in, stat_far, known, table,
    k_sem, f_sem, o_sem, send_sem, recv_sem, ready
):
    (images, height, width, wide, channels, outputs, group, depth, pixel_total) = sizes
    rows = images * height * wide
    kp = fp.shape[0]
    groups = channels // group
    blocks = channels // LANES
    tiles = 9
    taps = 3 * outputs
    quarter = group // 2
    plane = groups // depth
    image_rows = height * wide
    packed = quarter // 2

    batch = lax.axis_index("batch")
    row = lax.axis_index("rows")
    core = row % PAIR
    x = row // PAIR
    y = batch % SHALLOW
    z = batch // SHALLOW
    chip = (z * SHALLOW + y) * SHALLOW + x
    znear = z + 1 - 2 * (z % 2)
    zother = depth - 1 - z
    outer = (z == 0) | (z == depth - 1)
    inner = (z > 0) & (z < depth - 1)

    def place(x, y, z, core=core):
        return (z * SHALLOW + y, x * PAIR + core)

    partner = place(x, y, z, 1 - core)
    xside = place(1 - x, y, z)
    yside = place(x, 1 - y, z)

    def peer(k):
        px = 1 - x if k % 2 else x
        py = 1 - y if k // 2 % 2 else y
        low = 1 - z % 2 if k // 4 % 2 else z % 2
        high = 1 - z // 2 if k // 8 % 2 else z // 2
        pz = high * 2 + low
        return px, py, pz

    barrier = pltpu.get_barrier_semaphore()
    mesh_id = pl.DeviceIdType.MESH
    near = [xside, yside, place(x, y, znear)]
    count = len(near) + inner.astype(jnp.int32)

    def tell(sem, devices):
        for other in devices:
            pl.semaphore_signal(sem, inc=1, device_id=other, device_id_type=mesh_id)

        @pl.when(inner)
        def _():
            pl.semaphore_signal(
                sem, inc=1, device_id=place(x, y, zother), device_id_type=mesh_id
            )

    def spread(k):
        if k > 0:
            pl.semaphore_wait(ready.at[k - 1], count)
        tell(ready.at[k], near)

    def spread_done():
        pl.semaphore_wait(ready.at[3], count)

    tell(barrier, near + [partner])
    k_copy = pltpu.make_async_copy(k_hbm, k_ref, k_sem)
    g_copy = pltpu.make_async_copy(g_hbm, g_ref, f_sem.at[0])
    f_copy = pltpu.make_async_copy(f_hbm, f_ref, f_sem.at[1])
    v_copy = pltpu.make_async_copy(v_hbm, v_ref, f_sem.at[2])
    val_copy = pltpu.make_async_copy(val_hbm, val_ref, f_sem.at[3])
    for load in (g_copy, f_copy, v_copy, val_copy):
        load.start()

    sems = {}

    def copy(key, src, dst, device, landing=None):
        at = sems.setdefault(key, len(sems))
        to = at if landing is None else sems.setdefault(landing, len(sems))
        return pltpu.make_async_remote_copy(
            src_ref=src, dst_ref=dst, send_sem=send_sem.at[at], recv_sem=recv_sem.at[to],
            device_id=device, device_id_type=pl.DeviceIdType.MESH,
        )

    flights = {}

    def send(key, src, dst, device):
        flights[key] = copy(key, src, dst, device)
        flights[key].start()

    def arrive(key):
        flights.pop(key).wait()

    fp[pl.ds(rows, kp - rows), :] = jnp.zeros((kp - rows, channels), BF16)
    cols[pl.ds(rows, kp - rows), :] = jnp.zeros((kp - rows, 3 * taps), BF16)
    gpad[...] = jnp.zeros(gpad.shape, F32)

    g_copy.wait()

    @pl.loop(0, images)
    def _(b):
        gpad[pl.ds(1, height), pl.ds(1, width), :] = g_ref[b].astype(F32)
        at = pl.multiple_of(b * image_rows, 16)
        for c in range(3):
            shifted = gpad[:, 2 - c : 2 - c + wide, :].astype(BF16)
            for a in range(3):
                first = a * taps + c * outputs
                cols[pl.ds(at, image_rows), first : first + outputs] = shifted[
                    2 - a : 2 - a + height
                ].reshape(image_rows, outputs)

    f_copy.wait()
    k_copy.start()

    @pl.loop(0, images)
    def _(b):
        for h in range(height):
            at = pl.multiple_of((b * height + h) * wide, 16)
            fp[pl.ds(at, wide), :] = jnp.zeros((wide, channels), BF16)
            fp[pl.ds(at, width), :] = f_ref[b, h]

    @pl.loop(0, blocks)
    def _(k):
        at = pl.ds(pl.multiple_of(k * LANES, LANES), LANES)
        ft[at, :] = fp[:, at].T

    position = lax.broadcasted_iota(jnp.int32, (kp, 1), 0)
    valid = (position % wide < width) & (position < rows)
    lane = lax.broadcasted_iota(jnp.int32, (16, kp), 1)
    ft[pl.ds(channels, 16), :] = jnp.where(
        (lane % wide < width) & (lane < rows), 1.0, 0.0
    ).astype(BF16)
    stat[:, :, pl.ds(packed, 8), :] = jnp.zeros((PAIR, groups, 8, LANES), F32)

    first_plane = [0, 2, 4, 5, 6, 7, 8]
    first_depth = [1, 3]

    def slot(t, half, g):
        gz, gy, gx = g // 4, g // 2 % 2, g % 2
        first, second = (gx, gy) if half == 0 else (gy, gx)
        if t in first_depth:
            return gz * 4 + first * 2 + second
        return first * 8 + second * 4 + gz

    def tile(t):
        high = channels // 2
        for m in range(2):
            extra = 16 if m == 1 else 0
            part = jnp.dot(
                ft[m * high : (m + 1) * high + extra, :],
                cols[:, t * outputs : (t + 1) * outputs],
                preferred_element_type=F32,
            )
            for q in range(groups // 2):
                g = m * (groups // 2) + q
                for half in range(2):
                    lines = slice(q * group + half * quarter, q * group + (half + 1) * quarter)
                    for c in range(PAIR):
                        parts[t, c, half, slot(t, half, g)] = part[
                            lines, c * LANES : (c + 1) * LANES
                        ]
            if m == 1:
                for c in range(PAIR):
                    stat[c, t, packed + 1 : packed + 2, :] = part[
                        high : high + 1, c * LANES : (c + 1) * LANES
                    ]
        send(("swap", t), parts.at[t, 1 - core], swap.at[t], partner)

    def add(dst, src, dst_first, count, src_first=0):
        for i in range(count):
            dst[dst_first + i] = dst[dst_first + i] + src[src_first + i]

    def mine(t, half):
        return parts.at[t, core, half]

    firsts = [(x, y), (y, x)]
    sides = [(xside, yside), (yside, xside)]

    def swapped(t):
        arrive(("swap", t))
        for half in range(2):
            dst, src = mine(t, half), swap.at[t, half]

            @pl.loop(0, groups, step=8)
            def _(i):
                for j in range(8):
                    dst[i + j] = dst[i + j] + src[i + j]

    def plane1(t):
        for half in range(2):
            send(
                ("p1", t, half),
                mine(t, half).at[pl.ds((1 - firsts[half][0]) * 8, 8)],
                near1.at[t, half], sides[half][0],
            )

    def plane2(t):
        for half in range(2):
            arrive(("p1", t, half))
            f, s = firsts[half]
            add(mine(t, half), near1.at[t, half], f * 8 + (1 - s) * 4, 4, (1 - s) * 4)
            send(
                ("p2", t, half),
                mine(t, half).at[pl.ds(f * 8 + (1 - s) * 4, 4)],
                near2.at[t, half], sides[half][1],
            )
        for half in range(2):
            f, s = firsts[half]
            add(mine(t, half), near1.at[t, half], f * 8 + s * 4, 4, s * 4)

    def depth1(t):
        for half in range(2):
            arrive(("p2", t, half))
            f, s = firsts[half]
            src = mine(t, half)
            for j in range(depth):
                zsum[t, j, pl.ds(half * quarter, quarter)] = (
                    src[f * 8 + s * 4 + j] + near2[t, half, j]
                )
        key = ("z1", t)

        @pl.when(outer)
        def _():
            copy(
                key, zsum.at[t, pl.ds((depth - 1 - z) // 3, 3)], zin.at[t], place(x, y, znear)
            ).start()

        @pl.when(inner)
        def _():
            copy(
                key, zsum.at[t, pl.ds(znear, 1)], zin.at[t, pl.ds(0, 1)], place(x, y, znear)
            ).start()

    def depth2(t):
        key = ("z1", t)

        @pl.when(outer)
        def _():
            near = place(x, y, znear)
            copy(key, zsum.at[t, pl.ds((depth - 1 - z) // 3, 3)], zin.at[t], near).wait_send()
            copy(key, zsum.at[t, pl.ds(0, 1)], zin.at[t, pl.ds(0, 1)], near).wait_recv()
            zsum[t, z] = zsum[t, z] + zin[t, 0]

        @pl.when(inner)
        def _():
            near = place(x, y, znear)
            copy(key, zsum.at[t, pl.ds(znear, 1)], zin.at[t, pl.ds(0, 1)], near).wait_send()
            copy(key, zsum.at[t, pl.ds(0, 3)], zin.at[t], near).wait_recv()
            for j in range(3):
                zsum[t, 2 - z + j] = zsum[t, 2 - z + j] + zin[t, j]
            copy(
                ("z2", t), zsum.at[t, pl.ds(zother, 1)], zfar.at[t], place(x, y, zother)
            ).start()
            zfin = 3 * (2 - z)
            copy(
                ("z3", t), zsum.at[t, pl.ds(zfin, 1)], zfar.at[t], place(x, y, zfin), ("z2", t)
            ).start()

    def depth3(t):
        @pl.when(inner)
        def _():
            copy(
                ("z2", t), zsum.at[t, pl.ds(zother, 1)], zfar.at[t], place(x, y, zother)
            ).wait_send()
            zfin = 3 * (2 - z)
            copy(
                ("z3", t), zsum.at[t, pl.ds(zfin, 1)], zfar.at[t], place(x, y, zfin), ("z2", t)
            ).wait_send()

        copy(
            ("z2", t), zsum.at[t, pl.ds(0, 1)], zfar.at[t], place(x, y, zother)
        ).wait_recv()
        total[t] = zsum[t, z] + zfar[t, 0]

    def early1_start(t, half):
        e = first_depth.index(t)
        key = ("e1", t, half)
        src = mine(t, half)

        @pl.when(outer)
        def _():
            copy(
                key, src.at[pl.ds((depth - 1 - z) // 3 * 4, 12)], early_in.at[e, half],
                place(x, y, znear),
            ).start()

        @pl.when(inner)
        def _():
            copy(
                key, src.at[pl.ds(znear * 4, 4)], early_in.at[e, half, pl.ds(0, 4)],
                place(x, y, znear),
            ).start()

    def early2_start(t, half):
        e = first_depth.index(t)
        key = ("e1", t, half)
        src = mine(t, half)
        buf = early_in.at[e, half]
        far = early_far.at[e, half]

        @pl.when(outer)
        def _():
            near = place(x, y, znear)
            copy(key, src.at[pl.ds((depth - 1 - z) // 3 * 4, 12)], buf, near).wait_send()
            copy(key, src.at[pl.ds(0, 4)], buf.at[pl.ds(0, 4)], near).wait_recv()
            add(src, buf, z * 4, 4)

        @pl.when(inner)
        def _():
            near = place(x, y, znear)
            copy(key, src.at[pl.ds(znear * 4, 4)], buf.at[pl.ds(0, 4)], near).wait_send()
            copy(key, src.at[pl.ds(0, 12)], buf, near).wait_recv()
            add(src, buf, (2 - z) * 4, 12)
            copy(
                ("e2", t, half), src.at[pl.ds(zother * 4, 4)], far, place(x, y, zother)
            ).start()
            zfin = 3 * (2 - z)
            copy(
                ("e3", t, half), src.at[pl.ds(zfin * 4, 4)], far, place(x, y, zfin),
                ("e2", t, half),
            ).start()

    def early3_start(t, half):
        e = first_depth.index(t)
        src = mine(t, half)
        far = early_far.at[e, half]

        @pl.when(inner)
        def _():
            copy(
                ("e2", t, half), src.at[pl.ds(zother * 4, 4)], far, place(x, y, zother)
            ).wait_send()
            zfin = 3 * (2 - z)
            copy(
                ("e3", t, half), src.at[pl.ds(zfin * 4, 4)], far, place(x, y, zfin),
                ("e2", t, half),
            ).wait_send()

        copy(("e2", t, half), src.at[pl.ds(0, 4)], far, place(x, y, zother)).wait_recv()
        add(src, far, z * 4, 4)
        send(
            ("e4", t, half),
            src.at[pl.ds(z * 4 + (1 - firsts[half][0]) * 2, 2)],
            early1.at[e, half], sides[half][0],
        )

    def early4_start(t, half):
        e = first_depth.index(t)
        arrive(("e4", t, half))
        f, s = firsts[half]
        src = mine(t, half)
        add(src, early1.at[e, half], z * 4 + f * 2, 2)
        send(
            ("e5", t, half),
            src.at[pl.ds(z * 4 + f * 2 + (1 - s), 1)],
            early2.at[e, half], sides[half][1],
        )

    def early5(t, half):
        e = first_depth.index(t)
        arrive(("e5", t, half))
        f, s = firsts[half]
        src = mine(t, half)
        total[t, pl.ds(half * quarter, quarter)] = (
            src[z * 4 + f * 2 + s] + early2[e, half, 0]
        )

    step = 2 * LANES
    half_rows = kp // 2
    low_lane = lax.broadcasted_iota(jnp.int32, (quarter, LANES), 1) < LANES // 2
    low_line = lax.broadcasted_iota(jnp.int32, (8, LANES), 1) < LANES // 2

    def turn(a):
        return pltpu.roll(a, LANES // 2, 1)

    def back_part(n, r):
        at = slice(n * step, (n + 1) * step)
        here = slice(r * half_rows, (r + 1) * half_rows)
        back[here, at] = jnp.dot(cols[here, :], k_ref[:, at], preferred_element_type=F32)

    def cov_part(n):
        at = slice(n * step, (n + 1) * step)
        grad = back[:, at]
        summed = jnp.broadcast_to(
            jnp.sum(jnp.where(valid, grad, 0.0), axis=0, keepdims=True), (8, step)
        )
        raw = jnp.dot(ft[at, :], grad.astype(BF16), preferred_element_type=F32)
        fsum = jnp.dot(ft[channels : channels + 16, :], fp[:, at], preferred_element_type=F32)[:8]
        for q in range(2):
            wide_at = slice(q * LANES, (q + 1) * LANES)
            block = raw[wide_at, wide_at]
            bs, fs = summed[:, wide_at], fsum[:, wide_at]
            g = (2 * n + q) * 2
            pieces = [block[i * quarter : (i + 1) * quarter] for i in range(4)]
            lower = jnp.where(low_lane, pieces[0], turn(pieces[1]))
            upper = jnp.where(low_lane, turn(pieces[2]), pieces[3])
            for c in range(PAIR):
                stat[c, g, :packed] = lower[c * packed : (c + 1) * packed]
                stat[c, g + 1, :packed] = upper[c * packed : (c + 1) * packed]
            stat[0, g, packed : packed + 1] = jnp.where(low_line, fs, turn(bs))[:1]
            stat[0, g + 1, packed : packed + 1] = jnp.where(low_line, turn(fs), bs)[:1]

    def stat1():
        send("s1", stat.at[1 - core], stat_in, partner)

    def stat2():
        arrive("s1")
        src = stat.at[core]
        add(src, stat_in, 0, groups)
        for k in range(1, groups):
            px, py, pz = peer(k)
            send(
                ("s2", k), src.at[(pz * SHALLOW + py) * SHALLOW + px], stat_far.at[k],
                place(px, py, pz),
            )

    def stat3():
        summed = stat[core, chip]
        for k in range(1, groups):
            arrive(("s2", k))
            summed = summed + stat_far[k]
        known[core] = summed
        send("s3", known.at[core], known.at[core], partner)

    def across(line):
        return jnp.broadcast_to(line, (LANES, LANES)).T[:group, :group]

    def hdot(a, b, dims):
        return lax.dot_general(
            a, b, (dims, ((), ())), precision=highest, preferred_element_type=F32
        )

    def stat4():
        arrive("s3")
        lines = jnp.concatenate([known[0, :packed], known[1, :packed]], axis=0)
        raw = jnp.concatenate([lines, turn(lines)], axis=0)[:, :group]
        both = jnp.broadcast_to(known[0, packed : packed + 1], (8, LANES))
        mean = both[:1] / pixel_total
        summed = turn(both)[:1, :group]
        cov = raw - across(mean) * summed
        v = v_ref[chip]
        vals = jnp.concatenate(
            [val_ref[pl.ds(chip, 1), :], jnp.ones((1, LANES - group), F32)], axis=1
        )
        scale = lax.rsqrt(vals)
        root = jnp.sqrt(vals)
        turned = hdot(v, cov, ((0,), (0,)))
        rotated = hdot(turned, v, ((1,), (0,)))
        symmetric = 0.5 * (rotated + rotated.T)
        factor = -(across(scale) * scale[:, :group]) / (across(root) + root[:, :group])
        inside = hdot(v, symmetric * factor, ((1,), (0,)))
        sigma = 2.0 / pixel_total * hdot(inside, v, ((1,), (1,)))
        own_ref[...] = hdot(v * scale[:, :group], v, ((1,), (1,))).astype(BF16)
        sigma = jnp.concatenate([sigma, jnp.zeros((group, LANES - group), F32)], axis=1)
        folded = jnp.where(low_lane, sigma[:quarter], turn(sigma[quarter:]))
        table[core, chip, :packed] = jnp.where(core == 0, folded[:packed], folded[packed:])
        table[core, chip, packed:] = known[core, packed:]
        table[core, chip, packed : packed + 1] = known[0, packed : packed + 1]
        src = table.at[core, chip]
        for k in range(1, groups):
            send(("s4", k), src, src, place(*peer(k)))

    def stat5():
        for k in range(1, groups):
            arrive(("s4", k))
        send("s5", table.at[core], table.at[core], partner)

    def stat6():
        arrive("s5")
        for k in range(blocks):
            folded = [
                jnp.concatenate([table[0, 2 * k + q, :packed], table[1, 2 * k + q, :packed]], axis=0)
                for q in range(2)
            ]
            s_ref[k] = jnp.concatenate(
                [
                    jnp.where(low_lane, folded[0], 0.0),
                    jnp.where(low_lane, turn(folded[0]), 0.0),
                    jnp.where(low_lane, 0.0, turn(folded[1])),
                    jnp.where(low_lane, 0.0, folded[1]),
                ],
                axis=0,
            ).astype(BF16)
            sums = [
                jnp.broadcast_to(table[0, 2 * k + q, packed : packed + 1], (8, LANES))
                for q in range(2)
            ]
            means[0, k] = jnp.where(low_line, sums[0], turn(sums[1])) / pixel_total
            means[1, k] = jnp.where(low_line, turn(sums[0]), sums[1]) / pixel_total

    def whiten_part(k):
        zero = jnp.zeros((group, LANES - group), F32)
        for q in range(2):
            g = 2 * k + q
            v = v_ref[g]
            scaled = v * lax.rsqrt(val_ref[g : g + 1, :])
            w = jnp.concatenate([hdot(scaled, v, ((1,), (1,))), zero], axis=1)
            if q == 1:
                w = turn(w)
            w_ref[k, q * group : (q + 1) * group, :] = w.astype(BF16)

    def final_part(b):
        here = pl.ds(pl.multiple_of(b * image_rows, 16), image_rows)
        for k in range(blocks):
            at = slice(k * LANES, (k + 1) * LANES)
            shifted = (back[here, at] - means[1, k, :1]).astype(BF16)
            centered = (fp[here, at].astype(F32) - means[0, k, :1]).astype(BF16)
            out = jnp.dot(shifted, w_ref[k], preferred_element_type=F32) + jnp.dot(
                centered, s_ref[k], preferred_element_type=F32
            )
            o_ref[b, :, :, at] = out.astype(BF16).reshape(height, wide, LANES)[:, :width]

    puts = []

    def put(b):
        puts.append(pltpu.make_async_copy(o_ref.at[b], o_hbm.at[b], o_sem.at[b]))
        puts[-1].start()

    def whitened(t):
        both = known[0, packed : packed + 1] / pixel_total
        mean = jnp.broadcast_to(both, (LANES, LANES)).T[:group]
        block = total[t] - mean * table[core, t, packed + 1 : packed + 2]
        one = block.astype(BF16)
        left = block - one.astype(F32)
        two = left.astype(BF16)
        three = (left - two.astype(F32)).astype(BF16)
        weight = own_ref[...]
        mixed[t] = sum(
            lax.dot_general(weight, a, (((0,), (0,)), ((), ())), preferred_element_type=F32)
            for a in (one, two, three)
        )
        send(("m", t), mixed.at[t, pl.ds((1 - core) * quarter, quarter)], mixed_in.at[t], partner)
        here = pl.ds(pl.multiple_of(core * LANES, LANES), LANES)
        share_ref[t, :, here] = mixed[t, pl.ds(core * quarter, quarter)]

    def finished(t):
        arrive(("m", t))
        there = pl.ds(pl.multiple_of((1 - core) * LANES, LANES), LANES)
        share_ref[t, :, there] = mixed_in[t]
        puts.append(
            pltpu.make_async_copy(share_ref.at[t], share_hbm.at[t], o_sem.at[images + t])
        )
        puts[-1].start()

    p = first_plane
    e = first_depth
    pl.semaphore_wait(barrier, count + 1)
    spread(0)
    tile(p[0])
    spread(1)
    tile(e[0])
    spread(2)
    tile(p[1])
    spread(3)
    swapped(p[0])
    plane1(p[0])
    tile(e[1])
    spread_done()
    swapped(e[0])
    early1_start(e[0], 0)
    early1_start(e[0], 1)
    tile(p[2])
    swapped(p[1])
    plane1(p[1])
    tile(p[3])
    swapped(e[1])
    early1_start(e[1], 0)
    early1_start(e[1], 1)
    tile(p[4])
    swapped(p[2])
    plane1(p[2])
    tile(p[5])
    swapped(p[3])
    plane1(p[3])
    tile(p[6])
    plane2(p[0])
    swapped(p[4])
    k_copy.wait()
    v_copy.wait()
    val_copy.wait()
    back_part(0, 0)
    back_part(0, 1)
    early2_start(e[0], 0)
    cov_part(0)
    plane1(p[4])
    back_part(1, 0)
    back_part(1, 1)
    plane2(p[2])
    cov_part(1)
    back_part(2, 0)
    early2_start(e[0], 1)
    back_part(2, 1)
    plane2(p[3])
    cov_part(2)
    back_part(3, 0)
    depth1(p[0])
    back_part(3, 1)
    early2_start(e[1], 0)
    cov_part(3)
    stat1()
    whiten_part(7)
    plane2(p[4])
    early3_start(e[0], 1)
    whiten_part(5)
    whiten_part(0)
    whiten_part(1)
    whiten_part(6)
    stat2()
    depth1(p[2])
    early3_start(e[0], 0)
    plane2(p[1])
    whiten_part(3)
    whiten_part(4)
    early2_start(e[1], 1)
    depth1(p[3])
    swapped(p[5])
    plane1(p[5])
    swapped(p[6])
    whiten_part(2)
    early3_start(e[1], 0)
    depth1(p[4])
    depth2(p[0])
    early4_start(e[0], 1)
    plane1(p[6])
    early4_start(e[0], 0)
    depth1(p[1])
    depth2(p[2])
    early3_start(e[1], 1)
    stat3()
    plane2(p[5])
    early4_start(e[1], 0)
    stat4()
    depth2(p[3])
    depth3(p[0])
    depth3(p[2])
    depth2(p[4])
    early5(e[0], 0)
    early5(e[0], 1)
    plane2(p[6])
    early4_start(e[1], 1)
    depth2(p[1])
    depth1(p[5])
    early5(e[1], 0)
    early5(e[1], 1)
    depth1(p[6])
    depth3(p[3])
    depth2(p[5])
    stat5()
    depth3(p[4])
    depth3(p[1])
    stat6()
    depth2(p[6])
    final_part(0)
    put(0)
    final_part(1)
    put(1)
    final_part(2)
    put(2)
    final_part(3)
    put(3)
    final_part(4)
    put(4)
    final_part(5)
    put(5)
    depth3(p[5])
    whitened(e[0])
    whitened(e[1])
    whitened(p[0])
    whitened(p[1])
    whitened(p[2])
    whitened(p[3])
    whitened(p[4])
    whitened(p[5])
    depth3(p[6])
    whitened(p[6])
    finished(e[0])
    finished(e[1])
    finished(p[0])
    finished(p[1])
    finished(p[2])
    finished(p[3])
    finished(p[4])
    finished(p[5])
    finished(p[6])
    for move in puts:
        move.wait()


def place_kernel(held, share, placed, given, page, sheet, sems):
    count = held.shape[0]
    pairs = [(share, sheet, given)]
    pairs += [(held.at[b], page.at[b], placed.at[b]) for b in range(count)]
    loads = [
        pltpu.make_async_copy(src, mid, sems.at[0, i]) for i, (src, mid, _) in enumerate(pairs)
    ]
    stores = [
        pltpu.make_async_copy(mid, dst, sems.at[1, i]) for i, (_, mid, dst) in enumerate(pairs)
    ]
    for load in loads:
        load.start()
    for load, store in zip(loads, stores):
        load.wait()
        store.start()
    for store in stores:
        store.wait()


def plan_local(shape, features, grads, kernel, vectors, values):
    images, height, width, channels = features.shape
    outputs = grads.shape[3]
    groups, group = values.shape
    devices = shape[0] * shape[1]
    depth = shape[0] // SHALLOW
    taps = 3 * outputs
    wide = round_up(width, 16)
    rows = images * height * wide
    kp = round_up(rows + 1, LANES)
    blocks = channels // LANES
    pixel_total = 1.0 * images * height * width * devices
    quarter = group // 2
    stat_rows = quarter // 2 + 8
    sizes = (images, height, width, wide, channels, outputs, group, depth, pixel_total)
    anywhere = pl.BlockSpec(memory_space=pl.ANY)
    sem_count = 192
    f32 = [
        (9, PAIR, 2, groups, quarter, LANES),
        (9, 2, groups, quarter, LANES),
        (9, 2, 8, quarter, LANES),
        (9, 2, 4, quarter, LANES),
        (9, depth, group, LANES),
        (9, 3, group, LANES),
        (9, 1, group, LANES),
        (2, 2, 12, quarter, LANES),
        (2, 2, 4, quarter, LANES),
        (2, 2, 2, quarter, LANES),
        (2, 2, 1, quarter, LANES),
        (9, group, LANES),
        (9, group, LANES),
        (9, quarter, LANES),
        (PAIR, groups, stat_rows, LANES),
        (groups, stat_rows, LANES),
        (groups, stat_rows, LANES),
        (PAIR, stat_rows, LANES),
        (PAIR, groups, stat_rows, LANES),
    ]
    held, share = pl.pallas_call(
        functools.partial(plan_kernel, sizes),
        out_shape=(
            jax.ShapeDtypeStruct(features.shape, BF16),
            jax.ShapeDtypeStruct((9, channels // devices, outputs), F32),
        ),
        in_specs=[anywhere] * 5,
        out_specs=(anywhere, anywhere),
        scratch_shapes=[
            pltpu.VMEM(features.shape, BF16),
            pltpu.VMEM(grads.shape, BF16),
            pltpu.VMEM(vectors.shape, F32),
            pltpu.VMEM(values.shape, F32),
            pltpu.VMEM(features.shape, BF16),
            pltpu.VMEM((9, channels // devices, outputs), F32),
            pltpu.VMEM((kp, channels), BF16),
            pltpu.VMEM((channels + 16, kp), BF16),
            pltpu.VMEM((kp, 3 * taps), BF16),
            pltpu.VMEM((height + 2, wide + 8, outputs), F32),
            pltpu.VMEM((3 * taps, channels), BF16),
            pltpu.VMEM((kp, channels), F32),
            pltpu.VMEM((blocks, LANES, LANES), BF16),
            pltpu.VMEM((group, group), BF16),
            pltpu.VMEM((blocks, LANES, LANES), BF16),
            pltpu.VMEM((2, blocks, 8, LANES), F32),
        ]
        + [pltpu.VMEM(s, F32) for s in f32]
        + [
            pltpu.SemaphoreType.DMA,
            pltpu.SemaphoreType.DMA((4,)),
            pltpu.SemaphoreType.DMA((images + 9,)),
            pltpu.SemaphoreType.DMA((sem_count,)),
            pltpu.SemaphoreType.DMA((sem_count,)),
            pltpu.SemaphoreType.REGULAR((4,)),
        ],
        compiler_params=pltpu.CompilerParams(
            collective_id=0, has_side_effects=True, vmem_limit_bytes=VMEM_LIMIT
        ),
        name="step",
    )(features, grads, kernel.reshape(3 * taps, channels), vectors, values)
    per = channels // devices
    input_grad, share = pl.pallas_call(
        place_kernel,
        out_shape=(
            jax.ShapeDtypeStruct(features.shape, BF16),
            jax.ShapeDtypeStruct((9, per, outputs), F32),
        ),
        in_specs=[anywhere, anywhere],
        out_specs=(anywhere, anywhere),
        scratch_shapes=[
            pltpu.VMEM(features.shape, BF16),
            pltpu.VMEM((9, per, outputs), F32),
            pltpu.SemaphoreType.DMA((2, images + 1)),
        ],
        compiler_params=pltpu.CompilerParams(vmem_limit_bytes=VMEM_LIMIT),
        name="place",
    )(held, share)
    return (input_grad, share.reshape(3, 3, per, outputs).transpose(2, 0, 1, 3))


def solution(mesh):
    shape = (mesh.shape["batch"], mesh.shape["rows"])
    split = P(("batch", "rows"), None, None, None)

    def local(features, grads, kernel, vectors, values):
        groups, group = values.shape
        fits = (
            shape == (SHALLOW * 4, PAIR * SHALLOW)
            and groups * PAIR == shape[0] * shape[1]
            and group * 2 == LANES
            and grads.shape[3] == PAIR * LANES
            and features.shape[0] % 3 == 0
        )
        body = plan_local if fits else general_local
        return body(shape, features, grads, kernel, vectors, values)

    return jax.shard_map(
        local,
        mesh=mesh,
        in_specs=(split, split, P(), P(), P()),
        out_specs=(split, split),
        check_vma=False,
    )
```
